32 devices in a mesh: grp: 8 (over y, x, core), rep: 4 (over z).
Axes of the slice: x: 2, y: 2, z: 4, core: 2. Of those that a mesh axis runs over, the one named last changes fastest.
Arguments:
- momentum: bfloat16 [256, 4096], P(('grp', 'rep')), may hold values from -6 to 6
- picked: int32 [256, 32], P(('grp', 'rep')), may hold values from 0 to 4095, as said below
- owner_span_order: int32 [8], replicated, may hold values from 0 to 7, each once
Outputs:
- update: bfloat16 [8, 4096], replicated
- residual_momentum: bfloat16 [256, 4096], P(('grp', 'rep'))
The draws below stay inside these ranges and needn't reach their ends.
Inputs may be any that keep to these rules, and one draw needn't show every extreme that they name: `picked`: the 32 numbers of a row are different. `owner_span_order`: each span stands once.
All inputs are finite; a program needn't handle non-finite values.
Results may differ from the reference program's by a relative error of at most 0.013.
Values may be sent and summed in bfloat16 or wider, within the bound.
A program may use at most 64 MiB of HBM per device.

```python
import jax
import jax.numpy as jnp
from jax import lax

BLOCK = 64
COMP = 4096
TOPK = 32
SPANS = 8
DEVICES = 32


def draw_picked(key, part):
    streams = jax.random.split(jax.random.fold_in(key, 11), DEVICES)

    def one_device(stream):
        scores = jax.random.randint(stream, (SPANS, COMP), 0, 2 ** 18, dtype=jnp.int32) * COMP
        scores = scores + jnp.arange(COMP, dtype=jnp.int32)[None, :]
        return lax.top_k(scores, TOPK)[1].astype(jnp.int32)
    return lax.map(one_device, streams).reshape(DEVICES * SPANS, TOPK)


def block_scale(rng, extent, cuts, smallest, high):
    def one(position, blocks):
        draws = jax.random.uniform(jax.random.fold_in(jax.random.fold_in(rng, 6), position), (blocks,), jnp.float32, smallest / len(cuts), high / len(cuts))
        return jnp.repeat(jnp.exp(draws), extent[position] // blocks).reshape((-1,) + (1,) * (len(extent) - position - 1))

    gain = one(*cuts[0])
    for cut in cuts[1:]:
        gain = gain * one(*cut)
    return gain


def scatter_about(stream_key, shape, scale, limit, pieces=(), kind=jnp.bfloat16):
    drawn = jax.random.normal(stream_key, shape, jnp.float32) * scale
    if len(pieces) > 0:
        drawn = block_scale(stream_key, shape, pieces, -0.22, 0.18) * drawn
    return jnp.clip(drawn, min=-limit, max=limit).astype(kind)


def setup_inputs(seed: int = 0) -> dict:
    seeds = jax.random.split(jax.random.key(seed), 4)
    return {
        "momentum": scatter_about(seeds[0], (DEVICES * SPANS, COMP), 1.0, 6.0, ((0, 32),)),
        "picked": draw_picked(jax.random.fold_in(seeds[3], 71), 0),
        "owner_span_order": jax.random.permutation(seeds[2], SPANS).astype(jnp.int32),
    }


def dct_cosines(points):
    freq = jnp.arange(points, dtype=jnp.float32)[:, None]
    place = jnp.arange(points, dtype=jnp.float32)[None, :]
    values = jnp.cos(jnp.pi * (2.0 * place + 1.0) * freq / (2.0 * points)) * jnp.sqrt(2.0 / points)
    values = values.at[0].multiply(jnp.sqrt(0.5))
    rounded = lax.optimization_barrier(values.astype(jnp.bfloat16))
    return rounded.astype(jnp.float32)

def decode(dense_matrix, cosines):
    square = dense_matrix.reshape(dense_matrix.shape[0], BLOCK, BLOCK)
    half = jnp.einsum('cij,jb->cib', square, cosines, precision=lax.Precision.HIGHEST)
    full = jnp.einsum('ia,cib->cab', cosines, half, precision=lax.Precision.HIGHEST)
    return full.reshape(dense_matrix.shape[0], COMP)

def reference(momentum, picked, owner_span_order):
    cosines = dct_cosines(BLOCK)
    incoming_blocks = momentum.reshape(DEVICES, SPANS, COMP)
    picks = picked.reshape(DEVICES, SPANS, TOPK)
    span_rows = jnp.broadcast_to(jnp.arange(SPANS, dtype=jnp.int32)[:, None], (SPANS, TOPK))

    def accumulate_into(summed, input_list):
        momentum_dev, picks_dev = input_list
        square = momentum_dev.astype(jnp.float32).reshape(SPANS, BLOCK, BLOCK)
        half = jnp.einsum('cab,jb->caj', square, cosines, precision=lax.Precision.HIGHEST)
        freq_rows = cosines[picks_dev // BLOCK]
        freq_cols = cosines[picks_dev % BLOCK]
        half_cols = jnp.take_along_axis(half, (picks_dev % BLOCK)[:, None, :], axis=2)
        coeff_vals = jnp.einsum('cta,cat->ct', freq_rows, half_cols, precision=lax.Precision.HIGHEST)
        chosen = coeff_vals.astype(jnp.bfloat16).astype(jnp.float32)
        correction = jnp.einsum('cta,ctb->cab', freq_rows * chosen[:, :, None], freq_cols, precision=lax.Precision.HIGHEST)
        residual = (momentum_dev.astype(jnp.float32) - correction.reshape(SPANS, COMP)).astype(jnp.bfloat16)
        summed = summed.at[span_rows, picks_dev].add(chosen)
        return (summed, residual)
    summed, residuals = lax.scan(accumulate_into, jnp.zeros((SPANS, COMP), jnp.float32), (incoming_blocks, picks))
    decoded = decode(summed, cosines)
    update = decoded[owner_span_order].astype(jnp.bfloat16)
    return (update, residuals.reshape(DEVICES * SPANS, COMP))
```

```python
import math

import functools

import jax
import jax.numpy as jnp
from jax import lax
from jax.experimental import pallas as pl
from jax.experimental.pallas import tpu as pltpu
from jax.sharding import PartitionSpec as P

BLOCK = 64
TOPK = 32
CH_OWN = 1


def dct_cosines(points):
    freq = jnp.arange(points, dtype=jnp.float32)[:, None]
    place = jnp.arange(points, dtype=jnp.float32)[None, :]
    values = jnp.cos(jnp.pi * (2.0 * place + 1.0) * freq / (2.0 * points)) * jnp.sqrt(2.0 / points)
    values = values.at[0].multiply(jnp.sqrt(0.5))
    rounded = lax.optimization_barrier(values.astype(jnp.bfloat16))
    return rounded.astype(jnp.float32)


def forward(square_low, cosines, cos_low):
    half = jnp.einsum("cab,jb->caj", square_low, cos_low, preferred_element_type=jnp.float32)
    return jnp.einsum("ia,caj->cij", cosines, half, precision=lax.Precision.HIGHEST)


def decode(dense_matrix, cosines):
    square = dense_matrix.reshape(dense_matrix.shape[0], BLOCK, BLOCK)
    half = jnp.einsum("cij,jb->cib", square, cosines, precision=lax.Precision.HIGHEST)
    full = jnp.einsum("ia,cib->cab", cosines, half, precision=lax.Precision.HIGHEST)
    return full.reshape(dense_matrix.shape[0], BLOCK * BLOCK)


def decode_sparse(dense_low, cosines, cos_low):
    square = dense_low.reshape(dense_low.shape[0], BLOCK, BLOCK)
    half = jnp.einsum("cij,jb->cib", square, cos_low, preferred_element_type=jnp.float32)
    full = jnp.einsum("ia,cib->cab", cosines, half, precision=lax.Precision.HIGHEST)
    return full.reshape(dense_low.shape[0], BLOCK * BLOCK)


def densify(values, spots):
    entries, columns = values.shape
    per_step = math.gcd(entries, max(1, 65536 // columns))
    positions = jnp.arange(BLOCK, dtype=jnp.int32)

    def one_block(pieces):
        block_values, block_spots = pieces
        zeros = jnp.zeros_like(block_values)
        row_onehot = jnp.where(
            (block_spots // BLOCK)[:, None, :] == positions[None, :, None],
            block_values[:, None, :],
            zeros[:, None, :],
        )
        column_onehot = ((block_spots % BLOCK)[:, None, :] == positions[None, :, None]).astype(
            jnp.bfloat16
        )
        dense_matrix = jnp.einsum(
            "bcy,bzy->bcz", row_onehot, column_onehot, preferred_element_type=jnp.float32
        )
        return dense_matrix.reshape(per_step, BLOCK * BLOCK)

    stacked = lax.map(
        one_block,
        (
            values.reshape(entries // per_step, per_step, columns),
            spots.reshape(entries // per_step, per_step, columns),
        ),
    )
    return stacked.reshape(entries, BLOCK * BLOCK)


def owner_sum(received):
    values, spots = received
    return densify(values[0], spots[0])


def local_large(momentum, picked, owner_span_order):
    cosines = dct_cosines(BLOCK)
    cos_low = cosines.astype(jnp.bfloat16)
    owners = lax.axis_size("grp")
    span_count = momentum.shape[0]
    square_low = momentum.reshape(span_count, BLOCK, BLOCK)
    transform_coefficients = forward(square_low, cosines, cos_low).reshape(
        span_count, BLOCK * BLOCK
    )
    chosen = jnp.take_along_axis(transform_coefficients, picked, axis=1).astype(jnp.bfloat16)
    own_dense = densify(chosen, picked).astype(jnp.bfloat16)
    residual_momentum = (
        momentum.astype(jnp.float32) - decode_sparse(own_dense, cosines, cos_low)
    ).astype(jnp.bfloat16)
    slot_values = jnp.take(chosen, owner_span_order, axis=0)
    slot_spots = jnp.take(picked, owner_span_order, axis=0)
    shaped = (slot_values.reshape(owners, CH_OWN, TOPK), slot_spots.reshape(owners, CH_OWN, TOPK))
    partial_sum = owner_sum(
        (
            lax.all_to_all(shaped[0], "grp", split_axis=0, concat_axis=2, tiled=True),
            lax.all_to_all(shaped[1], "grp", split_axis=0, concat_axis=2, tiled=True),
        )
    )
    partial_sum = lax.psum(partial_sum, "rep")
    my_share = decode(partial_sum, cosines).astype(jnp.bfloat16)
    update = lax.all_gather(my_share, "grp", axis=0, tiled=True)
    return (update, residual_momentum)


LANES = 128
LOADS = 4
GATHER_BYTES = 2**20


def cosines_at(freq, place):
    turn = (freq * (2 * place + 1)) & (4 * BLOCK - 1)
    turn = jnp.where(turn > 2 * BLOCK, 4 * BLOCK - turn, turn)
    past = turn > BLOCK
    turn = jnp.where(past, 2 * BLOCK - turn, turn)
    angle = turn.astype(jnp.float32) * (math.pi / (2 * BLOCK))
    square = angle * angle
    value = jnp.full(square.shape, 1 / math.factorial(12), jnp.float32)
    for power in (10, 8, 6, 4, 2, 0):
        value = (-1) ** (power // 2) / math.factorial(power) + square * value
    scale = jnp.where(freq == 0, math.sqrt(1 / BLOCK), math.sqrt(2 / BLOCK))
    return (jnp.where(past, -value, value) * scale).astype(jnp.bfloat16)


def contract_lanes(left, right):
    return lax.dot_general(
        left, right, (((1,), (1,)), ((), ())), preferred_element_type=jnp.float32
    )


def matmul(left, right):
    return jnp.dot(left, right, preferred_element_type=jnp.float32)


def split(value):
    high = value.astype(jnp.bfloat16)
    return high, (value - high.astype(jnp.float32)).astype(jnp.bfloat16)


def exchange_kernel(
    groups,
    planes,
    order_hbm,
    momentum_hbm,
    picked_hbm,
    update_ref,
    residual_ref,
    order_ref,
    momentum_ref,
    picked_ref,
    rows_ref,
    cols_ref,
    twice_ref,
    pairs_ref,
    message,
    box,
    decoded,
    load_sem,
    send_sem,
    recv_sem,
    all_here,
):
    pltpu.make_async_copy(picked_hbm, picked_ref, load_sem.at[0]).start()
    pltpu.make_async_copy(order_hbm, order_ref, load_sem.at[1]).start()
    width = momentum_ref.shape[1] // LOADS
    for n in range(LOADS):
        piece = pl.ds(n * width, width)
        pltpu.make_async_copy(momentum_hbm.at[:, piece], momentum_ref.at[:, piece], load_sem.at[2]).start()
    spans = momentum_ref.shape[0]
    entries = spans * TOPK
    chunks = BLOCK * BLOCK // LANES
    folds = chunks // 2
    in_tile = LANES // TOPK
    tiles = entries // LANES
    halves = groups // in_tile
    devices = groups * planes
    my_group, my_plane = lax.axis_index("grp"), lax.axis_index("rep")
    group_of = [lax.rem(my_group + step, groups) for step in range(groups)]
    plane_of = [lax.rem(my_plane + step, planes) for step in range(planes)]
    first = {"grp": jnp.int32(0), "rep": jnp.int32(0)}
    second = {"grp": jnp.int32(1), "rep": jnp.int32(0)}
    is_first = jnp.logical_and(my_plane == 0, my_group == 0)
    is_second = jnp.logical_and(my_plane == 0, my_group == 1)
    last = {"grp": jnp.int32(groups - 1), "rep": jnp.int32(planes - 1)}
    is_last = jnp.logical_and(my_plane == planes - 1, my_group == groups - 1)
    is_early = jnp.logical_or(is_first, is_second)
    peers = [{"grp": group_of[g], "rep": plane_of[z]} for z in range(planes) for g in range(groups) if z or g]
    peers = peers[groups - 1 :] + peers[: groups - 1]
    barrier = pltpu.get_barrier_semaphore()

    def signal(semaphore, peer):
        pl.semaphore_signal(semaphore, inc=1, device_id=peer, device_id_type=pl.DeviceIdType.MESH)

    @pl.when(is_early)
    def _():
        for peer in peers:
            signal(barrier, peer)

    @pl.when(jnp.logical_not(jnp.logical_or(is_early, is_last)))
    def _():
        signal(barrier, last)

    def iotas(shape):
        return [lax.broadcasted_iota(jnp.int32, shape, d) for d in range(2)]

    line, freq = iotas((2 * folds * spans, BLOCK))
    place = 2 * (line % (folds * spans) // spans) + line // (folds * spans)
    rows_ref[...] = cosines_at(freq, place)
    line, freq = iotas((BLOCK, BLOCK))
    cols_ref[...] = cosines_at(freq, line)
    pairs_ref[...] = cosines_at(freq, 2 * (line % chunks) + line // chunks)
    line, place = iotas((BLOCK, LANES))
    twice_ref[...] = cosines_at(line, place % BLOCK)

    span, lane = iotas((spans, entries))
    turn = lax.rem(my_group, in_tile)
    block = (lane % LANES) // TOPK + in_tile - turn
    slot = lane // LANES * in_tile + jnp.where(block >= in_tile, block - in_tile, block)
    pltpu.make_async_copy(picked_hbm, picked_ref, load_sem.at[0]).wait()
    pltpu.make_async_copy(order_hbm, order_ref, load_sem.at[1]).wait()
    sent = jnp.full(slot.shape, order_ref[0])
    for s in range(1, spans):
        sent = jnp.where(slot == s, order_ref[s], sent)
    mine = span == sent
    spread = jnp.concatenate([picked_ref[...]] * spans, axis=1)
    spots = jnp.sum(jnp.where(mine, spread, 0), axis=0, keepdims=True)
    freq = lax.broadcasted_iota(jnp.int32, (BLOCK, entries), 0)
    row_spot, col_spot = spots // BLOCK, spots % BLOCK
    one_row = jnp.where(freq == row_spot, 1.0, 0.0).astype(jnp.bfloat16)
    one_col = jnp.where(freq == col_spot, 1.0, 0.0).astype(jnp.bfloat16)
    odd = jnp.where(row_spot % 2 == 1, -1.0, 1.0)
    wave = matmul(cols_ref[...], one_col)
    mirror = (wave * odd).astype(jnp.bfloat16)
    wave = wave.astype(jnp.bfloat16)
    blank = jnp.zeros_like(wave)
    waves = [
        jnp.concatenate([wave, blank, blank, mirror], axis=0),
        jnp.concatenate([blank, wave, mirror, blank], axis=0),
    ]
    half_rows = folds * spans
    row_waves = [matmul(rows_ref[p * half_rows : (p + 1) * half_rows, :], one_row) for p in range(2)]

    def by_tile(row):
        return jnp.concatenate(
            [row[:, h * LANES : (h + 1) * LANES] for h in range(tiles)], axis=0
        ).astype(jnp.bfloat16)

    message[:, LANES : 2 * LANES] = by_tile(row_spot.astype(jnp.float32))
    message[:, 2 * LANES :] = by_tile(col_spot.astype(jnp.float32))

    @pl.when(is_last)
    def _():
        pl.semaphore_wait(barrier, devices - 1)
        for peer in peers:
            signal(all_here, peer)

    pltpu.make_async_copy(momentum_hbm, momentum_ref, load_sem.at[2]).wait()

    def chunk(k):
        return momentum_ref[:, k * LANES : (k + 1) * LANES].astype(jnp.float32)

    def folded():
        return jnp.concatenate(
            [
                jnp.concatenate([chunk(k) for k in range(folds)], axis=0),
                jnp.concatenate([chunk(chunks - 1 - k) for k in range(folds)], axis=0),
            ],
            axis=1,
        )

    momentum_low = folded().astype(jnp.bfloat16)
    total = jnp.zeros((spans, entries), jnp.float32)
    for p in range(2):
        product = row_waves[p] * matmul(momentum_low, waves[p])
        total += jnp.sum(product.reshape(folds, spans, entries), axis=0)
    chosen = jnp.sum(jnp.where(mine, total, 0.0), axis=0, keepdims=True)
    message[:, :LANES] = by_tile(chosen)
    me = my_plane * groups + my_group
    landing = recv_sem.at[my_plane * halves + my_group // in_tile]

    def send(peer):
        copy = pltpu.make_async_remote_copy(
            src_ref=message,
            dst_ref=box.at[me],
            send_sem=send_sem,
            recv_sem=landing,
            device_id=peer,
            device_id_type=pl.DeviceIdType.MESH,
        )
        return copy

    @pl.when(jnp.logical_not(is_last))
    def _():
        pl.semaphore_wait(barrier, jnp.where(is_early, 1, 2))

    pl.when(jnp.logical_not(is_first))(lambda: send(first).start())
    pl.when(jnp.logical_not(is_second))(lambda: send(second).start())
    pltpu.make_async_copy(message, box.at[me], landing).start()

    chosen = chosen.astype(jnp.bfloat16).astype(jnp.float32)
    scaled = jnp.where(mine, chosen, 0.0)
    residual = folded()
    for p in range(2):
        weight = row_waves[p].reshape(folds, spans, entries) * scaled[None]
        for part in split(weight.reshape(half_rows, entries)):
            residual -= contract_lanes(part, waves[p])
    for k in range(folds):
        for n, at in enumerate((k, chunks - 1 - k)):
            residual_ref[:, at * LANES : (at + 1) * LANES] = residual[
                k * spans : (k + 1) * spans, n * LANES : (n + 1) * LANES
            ].astype(jnp.bfloat16)

    @pl.when(jnp.logical_not(is_last))
    def _():
        pl.semaphore_wait(all_here, 1)

    for z in reversed(range(planes)):
        for g in range(groups):
            if z:
                peer = {"grp": group_of[g], "rep": jnp.int32(z)}
                if g:
                    send(peer).start()
                else:
                    pl.when(my_plane != z)(lambda peer=peer: send(peer).start())
            elif g > 1:
                peer = {"grp": jnp.int32(g), "rep": jnp.int32(0)}
                pl.when(jnp.logical_or(my_plane != 0, my_group != g))(lambda peer=peer: send(peer).start())

    block = lax.broadcasted_iota(jnp.int32, (tiles, LANES), 1) // TOPK
    taken = [block == turn for turn in range(in_tile)]
    one, zero = jnp.ones((), jnp.bfloat16), jnp.zeros((), jnp.bfloat16)

    def arrived(z, half):
        first = z * groups + half * in_tile
        landed = box.at[pl.ds(first, in_tile)]
        pltpu.make_async_copy(landed, landed, recv_sem.at[z * halves + half]).wait()
        slots = [box[first + n].astype(jnp.float32) for n in range(in_tile)]
        return [[slot[:, n * LANES : (n + 1) * LANES] for slot in slots] for n in range(3)]

    def span_rows(parts, c):
        row = parts[0]
        for turn in range(1, in_tile):
            row = jnp.where(taken[(c + turn) % in_tile], parts[turn], row)
        return row

    plane_at = [jnp.where(2 * my_plane < planes, z, planes - 1 - z) for z in range(planes)]
    grouped = [[(z, half) for half in range(halves)] for z in plane_at[:-1]]
    grouped += [[(plane_at[-1], half)] for half in range(halves)]
    sums = [None] * spans
    for group in grouped:
        pieces = [arrived(z, half) for z, half in group]
        freq = lax.broadcasted_iota(jnp.int32, (BLOCK, len(group) * LANES), 0)
        freq = freq.astype(jnp.float32).astype(jnp.bfloat16)
        for c in range(in_tile):
            value, row, column = (
                jnp.concatenate([span_rows(piece[n], c) for piece in pieces], axis=1).astype(jnp.bfloat16)
                for n in range(3)
            )
            for h in range(tiles):
                left = jnp.where(freq == row[h : h + 1], one, zero)
                right = jnp.where(freq == column[h : h + 1], value[h : h + 1], zero)
                part = contract_lanes(left, right)
                s = h * in_tile + c
                sums[s] = part if sums[s] is None else sums[s] + part
    lower = lax.broadcasted_iota(jnp.int32, (chunks, LANES), 1) < BLOCK
    dense = [matmul(part.astype(jnp.bfloat16), twice_ref[...]).astype(jnp.bfloat16) for part in sums]
    for s in range(spans):
        full = matmul(pairs_ref[...], dense[s])
        decoded[pl.ds(s, chunks, stride=spans), :] = jnp.where(lower, full[:chunks], full[chunks:])
    for k in range(chunks):
        update_ref[:, k * LANES : (k + 1) * LANES] = decoded[
            k * spans : (k + 1) * spans, :
        ].astype(jnp.bfloat16)
    for _ in range(devices - 1):
        send(first).wait_send()


def store_kernel(update_ref, residual_ref, update_hbm, residual_hbm, sem):
    stores = [
        pltpu.make_async_copy(residual_ref, residual_hbm, sem.at[0]),
        pltpu.make_async_copy(update_ref, update_hbm, sem.at[1]),
    ]
    for store in stores:
        store.start()
    for store in stores:
        store.wait()


def local_small(groups, planes, momentum, picked, owner_span_order):
    spans = momentum.shape[0]
    chunks = BLOCK * BLOCK // LANES
    operands = [owner_span_order, momentum, picked]
    anywhere = pl.BlockSpec(memory_space=pl.ANY)
    vmem = pl.BlockSpec(memory_space=pltpu.VMEM)
    devices = groups * planes
    tile_shape = (spans * TOPK // LANES, 3 * LANES)
    results = pl.pallas_call(
        functools.partial(exchange_kernel, groups, planes),
        out_shape=[pltpu.VMEM(momentum.shape, jnp.bfloat16)] * 2,
        in_specs=[anywhere] * len(operands),
        out_specs=[vmem] * 2,
        scratch_shapes=[
            pltpu.SMEM(owner_span_order.shape, jnp.int32),
            pltpu.VMEM(momentum.shape, momentum.dtype),
            pltpu.VMEM(picked.shape, picked.dtype),
            pltpu.VMEM((chunks * spans, BLOCK), jnp.bfloat16),
            pltpu.VMEM((BLOCK, BLOCK), jnp.bfloat16),
            pltpu.VMEM((BLOCK, LANES), jnp.bfloat16),
            pltpu.VMEM((BLOCK, BLOCK), jnp.bfloat16),
            pltpu.VMEM(tile_shape, jnp.bfloat16),
            pltpu.VMEM((devices, *tile_shape), jnp.bfloat16),
            pltpu.VMEM((chunks * spans, LANES), jnp.float32),
            pltpu.SemaphoreType.DMA((3,)),
            pltpu.SemaphoreType.DMA,
            pltpu.SemaphoreType.DMA((devices * TOPK // LANES,)),
            pltpu.SemaphoreType.REGULAR,
        ],
        compiler_params=pltpu.CompilerParams(collective_id=0, has_side_effects=True),
    )(*operands)
    return pl.pallas_call(
        store_kernel,
        out_shape=[jax.ShapeDtypeStruct(momentum.shape, jnp.bfloat16)] * 2,
        in_specs=[vmem] * 2,
        out_specs=[anywhere] * 2,
        scratch_shapes=[pltpu.SemaphoreType.DMA((2,))],
    )(*[pltpu.with_memory_space_constraint(result, pltpu.VMEM) for result in results])


def local(groups, planes, momentum, picked, owner_span_order):
    entries = momentum.shape[0] * TOPK
    if entries % LANES == 0 and groups % (LANES // TOPK) == 0 and groups * planes * entries * 8 <= GATHER_BYTES:
        return local_small(groups, planes, momentum, picked, owner_span_order)
    return local_large(momentum, picked, owner_span_order)


def solution(mesh):
    return jax.shard_map(
        functools.partial(local, mesh.shape["grp"], mesh.shape["rep"]),
        mesh=mesh,
        in_specs=(P(("grp", "rep"), None), P(("grp", "rep"), None), P()),
        out_specs=(P(), P(("grp", "rep"), None)),
        check_vma=False,
    )
```

```python
import math

import functools

import jax
import jax.numpy as jnp
from jax import lax
from jax.experimental import pallas as pl
from jax.experimental.pallas import tpu as pltpu
from jax.sharding import PartitionSpec as P

BLOCK = 64
TOPK = 32
CH_OWN = 1


def dct_cosines(points):
    freq = jnp.arange(points, dtype=jnp.float32)[:, None]
    place = jnp.arange(points, dtype=jnp.float32)[None, :]
    values = jnp.cos(jnp.pi * (2.0 * place + 1.0) * freq / (2.0 * points)) * jnp.sqrt(2.0 / points)
    values = values.at[0].multiply(jnp.sqrt(0.5))
    rounded = lax.optimization_barrier(values.astype(jnp.bfloat16))
    return rounded.astype(jnp.float32)


def forward(square_low, cosines, cos_low):
    half = jnp.einsum("cab,jb->caj", square_low, cos_low, preferred_element_type=jnp.float32)
    return jnp.einsum("ia,caj->cij", cosines, half, precision=lax.Precision.HIGHEST)


def decode(dense_matrix, cosines):
    square = dense_matrix.reshape(dense_matrix.shape[0], BLOCK, BLOCK)
    half = jnp.einsum("cij,jb->cib", square, cosines, precision=lax.Precision.HIGHEST)
    full = jnp.einsum("ia,cib->cab", cosines, half, precision=lax.Precision.HIGHEST)
    return full.reshape(dense_matrix.shape[0], BLOCK * BLOCK)


def decode_sparse(dense_low, cosines, cos_low):
    square = dense_low.reshape(dense_low.shape[0], BLOCK, BLOCK)
    half = jnp.einsum("cij,jb->cib", square, cos_low, preferred_element_type=jnp.float32)
    full = jnp.einsum("ia,cib->cab", cosines, half, precision=lax.Precision.HIGHEST)
    return full.reshape(dense_low.shape[0], BLOCK * BLOCK)


def densify(values, spots):
    entries, columns = values.shape
    per_step = math.gcd(entries, max(1, 65536 // columns))
    positions = jnp.arange(BLOCK, dtype=jnp.int32)

    def one_block(pieces):
        block_values, block_spots = pieces
        zeros = jnp.zeros_like(block_values)
        row_onehot = jnp.where(
            (block_spots // BLOCK)[:, None, :] == positions[None, :, None],
            block_values[:, None, :],
            zeros[:, None, :],
        )
        column_onehot = ((block_spots % BLOCK)[:, None, :] == positions[None, :, None]).astype(
            jnp.bfloat16
        )
        dense_matrix = jnp.einsum(
            "bcy,bzy->bcz", row_onehot, column_onehot, preferred_element_type=jnp.float32
        )
        return dense_matrix.reshape(per_step, BLOCK * BLOCK)

    stacked = lax.map(
        one_block,
        (
            values.reshape(entries // per_step, per_step, columns),
            spots.reshape(entries // per_step, per_step, columns),
        ),
    )
    return stacked.reshape(entries, BLOCK * BLOCK)


def owner_sum(received):
    values, spots = received
    return densify(values[0], spots[0])


def local_large(momentum, picked, owner_span_order):
    cosines = dct_cosines(BLOCK)
    cos_low = cosines.astype(jnp.bfloat16)
    owners = lax.axis_size("grp")
    span_count = momentum.shape[0]
    square_low = momentum.reshape(span_count, BLOCK, BLOCK)
    transform_coefficients = forward(square_low, cosines, cos_low).reshape(
        span_count, BLOCK * BLOCK
    )
    chosen = jnp.take_along_axis(transform_coefficients, picked, axis=1).astype(jnp.bfloat16)
    own_dense = densify(chosen, picked).astype(jnp.bfloat16)
    residual_momentum = (
        momentum.astype(jnp.float32) - decode_sparse(own_dense, cosines, cos_low)
    ).astype(jnp.bfloat16)
    slot_values = jnp.take(chosen, owner_span_order, axis=0)
    slot_spots = jnp.take(picked, owner_span_order, axis=0)
    shaped = (slot_values.reshape(owners, CH_OWN, TOPK), slot_spots.reshape(owners, CH_OWN, TOPK))
    partial_sum = owner_sum(
        (
            lax.all_to_all(shaped[0], "grp", split_axis=0, concat_axis=2, tiled=True),
            lax.all_to_all(shaped[1], "grp", split_axis=0, concat_axis=2, tiled=True),
        )
    )
    partial_sum = lax.psum(partial_sum, "rep")
    my_share = decode(partial_sum, cosines).astype(jnp.bfloat16)
    update = lax.all_gather(my_share, "grp", axis=0, tiled=True)
    return (update, residual_momentum)


LANES = 128
LOADS = 4
EARLY = 2
GATHER_BYTES = 2**20


def cosines_at(freq, place):
    turn = (freq * (2 * place + 1)) & (4 * BLOCK - 1)
    turn = jnp.where(turn > 2 * BLOCK, 4 * BLOCK - turn, turn)
    past = turn > BLOCK
    turn = jnp.where(past, 2 * BLOCK - turn, turn)
    angle = turn.astype(jnp.float32) * (math.pi / (2 * BLOCK))
    square = angle * angle
    value = jnp.full(square.shape, 1 / math.factorial(12), jnp.float32)
    for power in (10, 8, 6, 4, 2, 0):
        value = (-1) ** (power // 2) / math.factorial(power) + square * value
    scale = jnp.where(freq == 0, math.sqrt(1 / BLOCK), math.sqrt(2 / BLOCK))
    return (jnp.where(past, -value, value) * scale).astype(jnp.bfloat16)


def contract_lanes(left, right):
    return lax.dot_general(
        left, right, (((1,), (1,)), ((), ())), preferred_element_type=jnp.float32
    )


def matmul(left, right):
    return jnp.dot(left, right, preferred_element_type=jnp.float32)


def split(value):
    high = value.astype(jnp.bfloat16)
    return high, (value - high.astype(jnp.float32)).astype(jnp.bfloat16)


def exchange_kernel(
    groups,
    planes,
    order_hbm,
    momentum_hbm,
    picked_hbm,
    update_ref,
    residual_ref,
    order_ref,
    momentum_ref,
    picked_ref,
    rows_ref,
    wide_ref,
    twice_ref,
    pairs_ref,
    message,
    box,
    dense,
    decoded,
    load_sem,
    send_sem,
    recv_sem,
    all_here,
):
    pltpu.make_async_copy(picked_hbm, picked_ref, load_sem.at[0]).start()
    pltpu.make_async_copy(order_hbm, order_ref, load_sem.at[1]).start()
    width = momentum_ref.shape[1] // LOADS
    for n in range(LOADS):
        piece = pl.ds(n * width, width)
        pltpu.make_async_copy(momentum_hbm.at[:, piece], momentum_ref.at[:, piece], load_sem.at[2]).start()
    spans = momentum_ref.shape[0]
    entries = spans * TOPK
    chunks = BLOCK * BLOCK // LANES
    folds = chunks // 2
    in_tile = LANES // TOPK
    tiles = entries // LANES
    halves = groups // in_tile
    devices = groups * planes
    my_group, my_plane = lax.axis_index("grp"), lax.axis_index("rep")
    group_of = [lax.rem(my_group + step, groups) for step in range(groups)]
    early = max(1, planes * EARLY // 4)
    last = {"grp": jnp.int32(groups - 1), "rep": jnp.int32(planes - 1)}
    is_last = jnp.logical_and(my_plane == planes - 1, my_group == groups - 1)
    is_early = my_plane < early

    def each_peer(lowest, highest, action):
        for z in range(lowest, highest):
            for g in range(groups):
                peer = {"grp": group_of[g], "rep": jnp.int32(z)}
                if g:
                    action(peer)
                else:
                    pl.when(my_plane != z)(functools.partial(action, peer))

    barrier = pltpu.get_barrier_semaphore()

    def signal(semaphore, peer):
        pl.semaphore_signal(semaphore, inc=1, device_id=peer, device_id_type=pl.DeviceIdType.MESH)

    @pl.when(is_early)
    def _():
        each_peer(0, planes, functools.partial(signal, barrier))

    @pl.when(jnp.logical_not(jnp.logical_or(is_early, is_last)))
    def _():
        signal(barrier, last)

    def iotas(shape):
        return [lax.broadcasted_iota(jnp.int32, shape, d) for d in range(2)]

    line, freq = iotas((2 * folds, LANES))
    table = cosines_at(freq % BLOCK, 2 * (line % folds) + line // folds).astype(jnp.float32)
    for k in range(2 * folds):
        rows_ref[k * spans : (k + 1) * spans, :] = jnp.broadcast_to(table[k : k + 1], (spans, LANES))
    line, freq = iotas((BLOCK, BLOCK))
    pairs_ref[...] = cosines_at(freq, 2 * (line % chunks) + line // chunks)
    line, place = iotas((BLOCK, LANES))
    twice_ref[...] = cosines_at(line, place % BLOCK)
    wide_ref[...] = cosines_at(place % BLOCK, line).astype(jnp.float32)

    span, lane = iotas((spans, entries))
    turn = lax.rem(my_group, in_tile)
    block = (lane % LANES) // TOPK + in_tile - turn
    slot = lane // LANES * in_tile + jnp.where(block >= in_tile, block - in_tile, block)
    mine = span == slot

    @pl.when(is_last)
    def _():
        pl.semaphore_wait(barrier, devices - 1)
        each_peer(0, planes, functools.partial(signal, all_here))

    pltpu.make_async_copy(picked_hbm, picked_ref, load_sem.at[0]).wait()
    spread = jnp.concatenate([picked_ref[...]] * spans, axis=1)
    pltpu.make_async_copy(momentum_hbm, momentum_ref, load_sem.at[2]).wait()
    spots = jnp.sum(jnp.where(mine, spread, 0), axis=0, keepdims=True)
    row_spot, col_spot = spots // BLOCK, spots % BLOCK

    def looked_up(table, spot):
        height = table.shape[0]
        return jnp.concatenate(
            [
                jnp.take_along_axis(
                    table,
                    jnp.broadcast_to(spot[:, h * LANES : (h + 1) * LANES], (height, LANES)),
                    axis=1,
                    mode="promise_in_bounds",
                )
                for h in range(tiles)
            ],
            axis=1,
        )

    odd = jnp.where(row_spot % 2 == 1, -1.0, 1.0)
    wave = looked_up(wide_ref[...], col_spot)
    mirror = (wave * odd).astype(jnp.bfloat16)
    wave = wave.astype(jnp.bfloat16)
    blank = jnp.zeros_like(wave)
    waves = [
        jnp.concatenate([wave, blank, blank, mirror], axis=0),
        jnp.concatenate([blank, wave, mirror, blank], axis=0),
    ]
    half_rows = folds * spans
    row_waves = [looked_up(rows_ref[p * half_rows : (p + 1) * half_rows, :], row_spot) for p in range(2)]

    def by_tile(row):
        return jnp.concatenate(
            [row[:, h * LANES : (h + 1) * LANES] for h in range(tiles)], axis=0
        ).astype(jnp.bfloat16)

    message[:, LANES : 2 * LANES] = by_tile(row_spot.astype(jnp.float32))
    message[:, 2 * LANES :] = by_tile(col_spot.astype(jnp.float32))

    def chunk(k):
        return momentum_ref[:, k * LANES : (k + 1) * LANES].astype(jnp.float32)

    def folded():
        return jnp.concatenate(
            [
                jnp.concatenate([chunk(k) for k in range(folds)], axis=0),
                jnp.concatenate([chunk(chunks - 1 - k) for k in range(folds)], axis=0),
            ],
            axis=1,
        )

    momentum_low = folded().astype(jnp.bfloat16)
    total = jnp.zeros((spans, entries), jnp.float32)
    for p in range(2):
        product = row_waves[p] * matmul(momentum_low, waves[p])
        total += jnp.sum(product.reshape(folds, spans, entries), axis=0)
    chosen = jnp.sum(jnp.where(mine, total, 0.0), axis=0, keepdims=True)
    message[:, :LANES] = by_tile(chosen)
    me = my_plane * groups + my_group
    landing = recv_sem.at[my_plane * halves + my_group // in_tile]

    def copy_to(peer):
        return pltpu.make_async_remote_copy(
            src_ref=message,
            dst_ref=box.at[me],
            send_sem=send_sem,
            recv_sem=landing,
            device_id=peer,
            device_id_type=pl.DeviceIdType.MESH,
        )

    def send(peer):
        copy_to(peer).start()

    @pl.when(jnp.logical_not(is_last))
    def _():
        pl.semaphore_wait(barrier, jnp.where(is_early, early * groups - 1, early * groups))

    each_peer(0, early, send)
    pltpu.make_async_copy(message, box.at[me], landing).start()

    pltpu.make_async_copy(order_hbm, order_ref, load_sem.at[1]).wait()
    chosen = chosen.astype(jnp.bfloat16).astype(jnp.float32)
    scaled = jnp.where(mine, chosen, 0.0)
    residual = folded()
    for p in range(2):
        weight = row_waves[p].reshape(folds, spans, entries) * scaled[None]
        for part in split(weight.reshape(half_rows, entries)):
            residual -= contract_lanes(part, waves[p])
    for k in range(folds):
        for n, at in enumerate((k, chunks - 1 - k)):
            residual_ref[:, at * LANES : (at + 1) * LANES] = residual[
                k * spans : (k + 1) * spans, n * LANES : (n + 1) * LANES
            ].astype(jnp.bfloat16)

    @pl.when(jnp.logical_not(is_last))
    def _():
        pl.semaphore_wait(all_here, 1)

    each_peer(early, planes, send)

    block = lax.broadcasted_iota(jnp.int32, (tiles, LANES), 1) // TOPK
    taken = [block == turn for turn in range(in_tile)]
    one, zero = jnp.ones((), jnp.bfloat16), jnp.zeros((), jnp.bfloat16)

    def arrived(z, half):
        first = z * groups + half * in_tile
        landed = box.at[pl.ds(first, in_tile)]
        pltpu.make_async_copy(landed, landed, recv_sem.at[z * halves + half]).wait()
        slots = [box[first + n].astype(jnp.float32) for n in range(in_tile)]
        return [[slot[:, n * LANES : (n + 1) * LANES] for slot in slots] for n in range(3)]

    def span_rows(parts, c):
        row = parts[0]
        for turn in range(1, in_tile):
            row = jnp.where(taken[(c + turn) % in_tile], parts[turn], row)
        return row

    plane_at = [jnp.where(2 * my_plane < planes, z, planes - 1 - z) for z in range(planes)]
    grouped = [[(z, half) for half in range(halves)] for z in plane_at[:-1]]
    grouped += [[(plane_at[-1], half)] for half in range(halves)]
    sums = [None] * spans
    for group in grouped:
        pieces = [arrived(z, half) for z, half in group]
        freq = lax.broadcasted_iota(jnp.int32, (BLOCK, len(group) * LANES), 0)
        freq = freq.astype(jnp.float32).astype(jnp.bfloat16)
        for c in range(in_tile):
            value, row, column = (
                jnp.concatenate([span_rows(piece[n], c) for piece in pieces], axis=1).astype(jnp.bfloat16)
                for n in range(3)
            )
            for h in range(tiles):
                left = jnp.where(freq == row[h : h + 1], one, zero)
                right = jnp.where(freq == column[h : h + 1], value[h : h + 1], zero)
                part = contract_lanes(left, right)
                s = h * in_tile + c
                sums[s] = part if sums[s] is None else sums[s] + part
    lower = lax.broadcasted_iota(jnp.int32, (chunks, LANES), 1) < BLOCK
    for s in range(spans):
        dense[s] = matmul(sums[s].astype(jnp.bfloat16), twice_ref[...]).astype(jnp.bfloat16)
    for s in range(spans):
        full = matmul(pairs_ref[...], dense[order_ref[s]])
        decoded[pl.ds(s, chunks, stride=spans), :] = jnp.where(lower, full[:chunks], full[chunks:])
    for k in range(chunks):
        update_ref[:, k * LANES : (k + 1) * LANES] = decoded[
            k * spans : (k + 1) * spans, :
        ].astype(jnp.bfloat16)
    for _ in range(devices - 1):
        copy_to(last).wait_send()


def store_kernel(update_ref, residual_ref, update_hbm, residual_hbm, sem):
    stores = [
        pltpu.make_async_copy(residual_ref, residual_hbm, sem.at[0]),
        pltpu.make_async_copy(update_ref, update_hbm, sem.at[1]),
    ]
    for store in stores:
        store.start()
    for store in stores:
        store.wait()


def local_small(groups, planes, momentum, picked, owner_span_order):
    spans = momentum.shape[0]
    chunks = BLOCK * BLOCK // LANES
    operands = [owner_span_order, momentum, picked]
    anywhere = pl.BlockSpec(memory_space=pl.ANY)
    vmem = pl.BlockSpec(memory_space=pltpu.VMEM)
    devices = groups * planes
    tile_shape = (spans * TOPK // LANES, 3 * LANES)
    results = pl.pallas_call(
        functools.partial(exchange_kernel, groups, planes),
        out_shape=[pltpu.VMEM(momentum.shape, jnp.bfloat16)] * 2,
        in_specs=[anywhere] * len(operands),
        out_specs=[vmem] * 2,
        scratch_shapes=[
            pltpu.SMEM(owner_span_order.shape, jnp.int32),
            pltpu.VMEM(momentum.shape, momentum.dtype),
            pltpu.VMEM(picked.shape, picked.dtype),
            pltpu.VMEM((chunks * spans, LANES), jnp.float32),
            pltpu.VMEM((BLOCK, LANES), jnp.float32),
            pltpu.VMEM((BLOCK, LANES), jnp.bfloat16),
            pltpu.VMEM((BLOCK, BLOCK), jnp.bfloat16),
            pltpu.VMEM(tile_shape, jnp.bfloat16),
            pltpu.VMEM((devices, *tile_shape), jnp.bfloat16),
            pltpu.VMEM((spans, BLOCK, LANES), jnp.bfloat16),
            pltpu.VMEM((chunks * spans, LANES), jnp.float32),
            pltpu.SemaphoreType.DMA((3,)),
            pltpu.SemaphoreType.DMA,
            pltpu.SemaphoreType.DMA((devices * TOPK // LANES,)),
            pltpu.SemaphoreType.REGULAR,
        ],
        compiler_params=pltpu.CompilerParams(collective_id=0, has_side_effects=True),
    )(*operands)
    return pl.pallas_call(
        store_kernel,
        out_shape=[jax.ShapeDtypeStruct(momentum.shape, jnp.bfloat16)] * 2,
        in_specs=[vmem] * 2,
        out_specs=[anywhere] * 2,
        scratch_shapes=[pltpu.SemaphoreType.DMA((2,))],
    )(*[pltpu.with_memory_space_constraint(result, pltpu.VMEM) for result in results])


def local(groups, planes, momentum, picked, owner_span_order):
    entries = momentum.shape[0] * TOPK
    if entries % LANES == 0 and groups % (LANES // TOPK) == 0 and groups * planes * entries * 8 <= GATHER_BYTES:
        return local_small(groups, planes, momentum, picked, owner_span_order)
    return local_large(momentum, picked, owner_span_order)


def solution(mesh):
    return jax.shard_map(
        functools.partial(local, mesh.shape["grp"], mesh.shape["rep"]),
        mesh=mesh,
        in_specs=(P(("grp", "rep"), None), P(("grp", "rep"), None), P()),
        out_specs=(P(), P(("grp", "rep"), None)),
        check_vma=False,
    )
```

```python
import math

import functools

import jax
import jax.numpy as jnp
from jax import lax
from jax.experimental import pallas as pl
from jax.experimental.pallas import tpu as pltpu
from jax.sharding import PartitionSpec as P

BLOCK = 64
TOPK = 32
CH_OWN = 1


def dct_cosines(points):
    freq = jnp.arange(points, dtype=jnp.float32)[:, None]
    place = jnp.arange(points, dtype=jnp.float32)[None, :]
    values = jnp.cos(jnp.pi * (2.0 * place + 1.0) * freq / (2.0 * points)) * jnp.sqrt(2.0 / points)
    values = values.at[0].multiply(jnp.sqrt(0.5))
    rounded = lax.optimization_barrier(values.astype(jnp.bfloat16))
    return rounded.astype(jnp.float32)


def forward(square_low, cosines, cos_low):
    half = jnp.einsum("cab,jb->caj", square_low, cos_low, preferred_element_type=jnp.float32)
    return jnp.einsum("ia,caj->cij", cosines, half, precision=lax.Precision.HIGHEST)


def decode(dense_matrix, cosines):
    square = dense_matrix.reshape(dense_matrix.shape[0], BLOCK, BLOCK)
    half = jnp.einsum("cij,jb->cib", square, cosines, precision=lax.Precision.HIGHEST)
    full = jnp.einsum("ia,cib->cab", cosines, half, precision=lax.Precision.HIGHEST)
    return full.reshape(dense_matrix.shape[0], BLOCK * BLOCK)


def decode_sparse(dense_low, cosines, cos_low):
    square = dense_low.reshape(dense_low.shape[0], BLOCK, BLOCK)
    half = jnp.einsum("cij,jb->cib", square, cos_low, preferred_element_type=jnp.float32)
    full = jnp.einsum("ia,cib->cab", cosines, half, precision=lax.Precision.HIGHEST)
    return full.reshape(dense_low.shape[0], BLOCK * BLOCK)


def densify(values, spots):
    entries, columns = values.shape
    per_step = math.gcd(entries, max(1, 65536 // columns))
    positions = jnp.arange(BLOCK, dtype=jnp.int32)

    def one_block(pieces):
        block_values, block_spots = pieces
        zeros = jnp.zeros_like(block_values)
        row_onehot = jnp.where(
            (block_spots // BLOCK)[:, None, :] == positions[None, :, None],
            block_values[:, None, :],
            zeros[:, None, :],
        )
        column_onehot = ((block_spots % BLOCK)[:, None, :] == positions[None, :, None]).astype(
            jnp.bfloat16
        )
        dense_matrix = jnp.einsum(
            "bcy,bzy->bcz", row_onehot, column_onehot, preferred_element_type=jnp.float32
        )
        return dense_matrix.reshape(per_step, BLOCK * BLOCK)

    stacked = lax.map(
        one_block,
        (
            values.reshape(entries // per_step, per_step, columns),
            spots.reshape(entries // per_step, per_step, columns),
        ),
    )
    return stacked.reshape(entries, BLOCK * BLOCK)


def owner_sum(received):
    values, spots = received
    return densify(values[0], spots[0])


def local_large(momentum, picked, owner_span_order):
    cosines = dct_cosines(BLOCK)
    cos_low = cosines.astype(jnp.bfloat16)
    owners = lax.axis_size("grp")
    span_count = momentum.shape[0]
    square_low = momentum.reshape(span_count, BLOCK, BLOCK)
    transform_coefficients = forward(square_low, cosines, cos_low).reshape(
        span_count, BLOCK * BLOCK
    )
    chosen = jnp.take_along_axis(transform_coefficients, picked, axis=1).astype(jnp.bfloat16)
    own_dense = densify(chosen, picked).astype(jnp.bfloat16)
    residual_momentum = (
        momentum.astype(jnp.float32) - decode_sparse(own_dense, cosines, cos_low)
    ).astype(jnp.bfloat16)
    slot_values = jnp.take(chosen, owner_span_order, axis=0)
    slot_spots = jnp.take(picked, owner_span_order, axis=0)
    shaped = (slot_values.reshape(owners, CH_OWN, TOPK), slot_spots.reshape(owners, CH_OWN, TOPK))
    partial_sum = owner_sum(
        (
            lax.all_to_all(shaped[0], "grp", split_axis=0, concat_axis=2, tiled=True),
            lax.all_to_all(shaped[1], "grp", split_axis=0, concat_axis=2, tiled=True),
        )
    )
    partial_sum = lax.psum(partial_sum, "rep")
    my_share = decode(partial_sum, cosines).astype(jnp.bfloat16)
    update = lax.all_gather(my_share, "grp", axis=0, tiled=True)
    return (update, residual_momentum)


LANES = 128
LOADS = 4
GATHER_BYTES = 2**20


def cosines_at(freq, place):
    turn = (freq * (2 * place + 1)) & (4 * BLOCK - 1)
    turn = jnp.where(turn > 2 * BLOCK, 4 * BLOCK - turn, turn)
    past = turn > BLOCK
    turn = jnp.where(past, 2 * BLOCK - turn, turn)
    angle = turn.astype(jnp.float32) * (math.pi / (2 * BLOCK))
    square = angle * angle
    value = jnp.full(square.shape, 1 / math.factorial(12), jnp.float32)
    for power in (10, 8, 6, 4, 2, 0):
        value = (-1) ** (power // 2) / math.factorial(power) + square * value
    scale = jnp.where(freq == 0, math.sqrt(1 / BLOCK), math.sqrt(2 / BLOCK))
    return (jnp.where(past, -value, value) * scale).astype(jnp.bfloat16)


def contract_lanes(left, right):
    return lax.dot_general(
        left, right, (((1,), (1,)), ((), ())), preferred_element_type=jnp.float32
    )


def matmul(left, right):
    return jnp.dot(left, right, preferred_element_type=jnp.float32)


def split(value):
    high = value.astype(jnp.bfloat16)
    return high, (value - high.astype(jnp.float32)).astype(jnp.bfloat16)


def exchange_kernel(
    groups,
    planes,
    order_hbm,
    momentum_hbm,
    picked_hbm,
    update_ref,
    residual_ref,
    order_ref,
    momentum_ref,
    picked_ref,
    rows_ref,
    wide_ref,
    twice_ref,
    pairs_ref,
    message,
    box,
    dense,
    summed,
    partial,
    row_side,
    column_side,
    weights,
    decoded,
    load_sem,
    send_sem,
    recv_sem,
    spot_sem,
    all_here,
):
    pltpu.make_async_copy(picked_hbm, picked_ref, load_sem.at[0]).start()
    pltpu.make_async_copy(order_hbm, order_ref, load_sem.at[1]).start()
    width = momentum_ref.shape[1] // LOADS
    for n in range(LOADS):
        piece = pl.ds(n * width, width)
        pltpu.make_async_copy(momentum_hbm.at[:, piece], momentum_ref.at[:, piece], load_sem.at[2]).start()
    spans = momentum_ref.shape[0]
    entries = spans * TOPK
    chunks = BLOCK * BLOCK // LANES
    folds = chunks // 2
    in_tile = LANES // TOPK
    tiles = entries // LANES
    halves = groups // in_tile
    devices = groups * planes
    my_group, my_plane = lax.axis_index("grp"), lax.axis_index("rep")
    group_of = [lax.rem(my_group + step, groups) for step in range(groups)]
    early_planes, early_groups = max(1, planes // 2), max(1, groups // 2)
    early = early_planes * early_groups
    last = {"grp": jnp.int32(groups - 1), "rep": jnp.int32(planes - 1)}
    hubs = 2
    is_hub = jnp.logical_and(my_plane == 0, my_group < hubs)
    is_final = jnp.logical_and(my_plane == planes - 1, my_group >= groups - in_tile)
    is_last = jnp.logical_and(my_plane == planes - 1, my_group == groups - 1)
    is_early = jnp.logical_and(my_plane < early_planes, my_group < early_groups)

    def to_all(planes_of, groups_of, action):
        for z in planes_of:
            for g in groups_of:
                peer = {"grp": jnp.int32(g), "rep": jnp.int32(z)}
                is_me = jnp.logical_and(my_plane == z, my_group == g)
                pl.when(jnp.logical_not(is_me))(functools.partial(action, peer))

    def to_hubs(action):
        to_all(range(1), range(hubs), action)

    def to_others(action):
        to_all(range(1), range(hubs, early_groups), action)
        to_all(range(1, early_planes), range(early_groups), action)

    def to_early(action):
        to_hubs(action)
        to_others(action)

    def to_late(action):
        for z in range(early_planes, planes):
            for g in range(groups):
                peer = {"grp": group_of[g], "rep": jnp.int32(z)}
                if g:
                    action(peer)
                else:
                    pl.when(my_plane != z)(functools.partial(action, peer))
        to_all(range(early_planes), range(early_groups, groups), action)

    barrier = pltpu.get_barrier_semaphore()

    def signal(semaphore, peer):
        pl.semaphore_signal(semaphore, inc=1, device_id=peer, device_id_type=pl.DeviceIdType.MESH)

    @pl.when(is_early)
    def _():
        to_late(functools.partial(signal, barrier))
        to_early(functools.partial(signal, barrier))

    @pl.when(jnp.logical_not(jnp.logical_or(is_early, is_last)))
    def _():
        signal(barrier, last)

    def iotas(shape):
        return [lax.broadcasted_iota(jnp.int32, shape, d) for d in range(2)]

    line, freq = iotas((2 * folds, LANES))
    rows_ref[...] = cosines_at(freq % BLOCK, 2 * (line % folds) + line // folds).astype(jnp.float32)
    line, freq = iotas((BLOCK, BLOCK))
    pairs_ref[...] = cosines_at(freq, 2 * (line % chunks) + line // chunks)
    line, place = iotas((BLOCK, LANES))
    twice_ref[...] = cosines_at(line, place % BLOCK)
    wide_ref[...] = cosines_at(place % BLOCK, line).astype(jnp.float32)

    span, lane = iotas((spans, entries))
    turn = lax.rem(my_group, in_tile)
    block = (lane % LANES) // TOPK + in_tile - turn
    slot = lane // LANES * in_tile + jnp.where(block >= in_tile, block - in_tile, block)
    mine = span == slot

    @pl.when(is_last)
    def _():
        pl.semaphore_wait(barrier, devices - 1)
        to_late(functools.partial(signal, all_here))
        to_early(functools.partial(signal, all_here))

    pltpu.make_async_copy(picked_hbm, picked_ref, load_sem.at[0]).wait()
    spread = jnp.concatenate([picked_ref[...]] * spans, axis=1)
    pltpu.make_async_copy(momentum_hbm, momentum_ref, load_sem.at[2]).wait()
    spots = jnp.sum(jnp.where(mine, spread, 0), axis=0, keepdims=True)
    row_spot, col_spot = spots // BLOCK, spots % BLOCK

    def looked_up(table, spot):
        height = table.shape[0]
        return jnp.concatenate(
            [
                jnp.take_along_axis(
                    table,
                    jnp.broadcast_to(spot[:, h * LANES : (h + 1) * LANES], (height, LANES)),
                    axis=1,
                    mode="promise_in_bounds",
                )
                for h in range(tiles)
            ],
            axis=1,
        )

    odd = jnp.where(row_spot % 2 == 1, -1.0, 1.0)
    wave = looked_up(wide_ref[...], col_spot)
    mirror = (wave * odd).astype(jnp.bfloat16)
    wave = wave.astype(jnp.bfloat16)
    waves = [jnp.concatenate([wave, mirror], axis=0), jnp.concatenate([mirror, wave], axis=0)]
    half_rows = folds * spans
    row_wave = looked_up(rows_ref[...], row_spot)
    row_waves = [row_wave[p * folds : (p + 1) * folds][:, None, :] for p in range(2)]

    def by_tile(row):
        return jnp.concatenate(
            [row[:, h * LANES : (h + 1) * LANES] for h in range(tiles)], axis=0
        ).astype(jnp.bfloat16)

    me = my_plane * groups + my_group
    landing = my_plane * halves + my_group // in_tile
    value_part, spot_part = pl.ds(0, LANES), pl.ds(LANES, 2 * LANES)

    def copy_to(peer, lanes, semaphore):
        return pltpu.make_async_remote_copy(
            src_ref=message.at[:, lanes],
            dst_ref=box.at[me, :, lanes],
            send_sem=send_sem,
            recv_sem=semaphore,
            device_id=peer,
            device_id_type=pl.DeviceIdType.MESH,
        )

    def send(peer):
        copy_to(peer, pl.ds(0, 3 * LANES), recv_sem.at[landing]).start()

    def send_spots(peer):
        copy_to(peer, spot_part, spot_sem).start()

    def send_values(peer):
        copy_to(peer, value_part, recv_sem.at[landing]).start()

    message[:, LANES : 2 * LANES] = by_tile(row_spot.astype(jnp.float32))
    message[:, 2 * LANES :] = by_tile(col_spot.astype(jnp.float32))
    @pl.when(jnp.logical_and(is_final, jnp.logical_not(is_last)))
    def _():
        pl.semaphore_wait(barrier, early)

    pl.when(is_final)(lambda: to_hubs(send_spots))

    def chunk(k):
        return momentum_ref[:, k * LANES : (k + 1) * LANES].astype(jnp.float32)

    left_lanes = lax.broadcasted_iota(jnp.int32, (spans, LANES), 1) < BLOCK

    def folded(p):
        pairs = [(chunk(k), chunk(chunks - 1 - k)) for k in range(folds)]
        return jnp.concatenate([jnp.where(left_lanes, pair[p], pair[1 - p]) for pair in pairs], axis=0)

    total = jnp.zeros((spans, entries), jnp.float32)
    for p in range(2):
        product = matmul(folded(p).astype(jnp.bfloat16), waves[p]).reshape(folds, spans, entries)
        total += jnp.sum(row_waves[p] * product, axis=0)
    chosen = jnp.sum(jnp.where(mine, total, 0.0), axis=0, keepdims=True)
    message[:, :LANES] = by_tile(chosen)

    @pl.when(jnp.logical_not(is_final))
    def _():
        pl.semaphore_wait(barrier, jnp.where(is_early, early - 1, early))
        to_hubs(send)

    pl.when(is_final)(lambda: to_hubs(send_values))
    to_others(send)

    pltpu.make_async_copy(message, box.at[me], recv_sem.at[landing]).start()

    pltpu.make_async_copy(order_hbm, order_ref, load_sem.at[1]).wait()
    chosen = chosen.astype(jnp.bfloat16).astype(jnp.float32)
    scaled = jnp.where(mine, chosen, 0.0)
    residuals = []
    for p in range(2):
        weight = row_waves[p] * scaled[None]
        residual = folded(p)
        for part in split(weight.reshape(half_rows, entries)):
            residual -= contract_lanes(part, waves[p])
        residuals.append(residual)
    for k in range(folds):
        pair = [residual[k * spans : (k + 1) * spans] for residual in residuals]
        for n, at in enumerate((k, chunks - 1 - k)):
            residual_ref[:, at * LANES : (at + 1) * LANES] = jnp.where(
                left_lanes, pair[n], pair[1 - n]
            ).astype(jnp.bfloat16)

    @pl.when(jnp.logical_not(is_last))
    def _():
        pl.semaphore_wait(all_here, 1)

    to_late(send)

    block = lax.broadcasted_iota(jnp.int32, (tiles, LANES), 1) // TOPK
    taken = [block == turn for turn in range(in_tile)]
    one, zero = jnp.ones((), jnp.bfloat16), jnp.zeros((), jnp.bfloat16)

    def await_part(z, half, lanes, semaphore):
        landed = box.at[pl.ds(z * groups + half * in_tile, in_tile), :, lanes]
        pltpu.make_async_copy(landed, landed, semaphore).wait()

    def parts_of(z, half, part):
        first = z * groups + half * in_tile
        lanes = slice(part * LANES, (part + 1) * LANES)
        return [box[first + n, :, lanes].astype(jnp.float32) for n in range(in_tile)]

    def arrived(z, half):
        await_part(z, half, pl.ds(0, 3 * LANES), recv_sem.at[z * halves + half])
        return [parts_of(z, half, part) for part in range(3)]

    def span_rows(parts, c):
        row = parts[0]
        for turn in range(1, in_tile):
            row = jnp.where(taken[(c + turn) % in_tile], parts[turn], row)
        return row

    plane_at = [jnp.where(2 * my_plane < planes, z, planes - 1 - z) for z in range(planes)]
    grouped = [[(z, half) for half in range(halves)] for z in plane_at]
    last_group = grouped.pop() if halves == 1 else [grouped[-1].pop()]

    def spread_out(row, freq, fill):
        return jnp.where(freq == row, fill, zero)

    def add_up(groups_of, start):
        sums = start
        for group in groups_of:
            if not group:
                continue
            pieces = [arrived(z, half) for z, half in group]
            freq = lax.broadcasted_iota(jnp.int32, (BLOCK, len(group) * LANES), 0)
            freq = freq.astype(jnp.float32).astype(jnp.bfloat16)
            for c in range(in_tile):
                value, row, column = (
                    jnp.concatenate([span_rows(piece[n], c) for piece in pieces], axis=1).astype(jnp.bfloat16)
                    for n in range(3)
                )
                for h in range(tiles):
                    left = spread_out(row[h : h + 1], freq, one)
                    right = spread_out(column[h : h + 1], freq, value[h : h + 1])
                    part = contract_lanes(left, right)
                    s = h * in_tile + c
                    sums[s] = part if sums[s] is None else sums[s] + part
        return sums

    lower = lax.broadcasted_iota(jnp.int32, (chunks, LANES), 1) < BLOCK

    def slot_matrices(sums):
        for s in range(spans):
            dense[s] = matmul(sums[s].astype(jnp.bfloat16), twice_ref[...]).astype(jnp.bfloat16)
        for s in range(spans):
            full = matmul(pairs_ref[...], dense[order_ref[s]])
            yield s, jnp.where(lower, full[:chunks], full[chunks:])

    for s, total in enumerate(add_up(grouped, [None] * spans)):
        summed[s] = total

    @pl.when(jnp.logical_not(is_hub))
    def _():
        for s, matrix in slot_matrices(add_up([last_group], [summed[s] for s in range(spans)])):
            decoded[pl.ds(s, chunks, stride=spans), :] = matrix

    @pl.when(is_hub)
    def _():
        for s, matrix in slot_matrices([summed[s] for s in range(spans)]):
            partial[s] = matrix
        final = (planes - 1, halves - 1)
        await_part(*final, spot_part, spot_sem)
        freq = lax.broadcasted_iota(jnp.int32, (BLOCK, entries), 0)
        freq = freq.astype(jnp.float32).astype(jnp.bfloat16)
        rows, columns = (parts_of(*final, part) for part in (1, 2))
        for c in range(in_tile):
            row, column = (
                jnp.concatenate([span_rows(parts, c)[h : h + 1] for h in range(tiles)], axis=1).astype(jnp.bfloat16)
                for parts in (rows, columns)
            )
            left = matmul(pairs_ref[...], spread_out(row, freq, one)).astype(jnp.bfloat16)
            right = matmul(wide_ref[:, :BLOCK].astype(jnp.bfloat16), spread_out(column, freq, one)).astype(jnp.bfloat16)
            for h in range(tiles):
                row_side[h * in_tile + c] = left[:, h * LANES : (h + 1) * LANES]
                column_side[h * in_tile + c] = right[:, h * LANES : (h + 1) * LANES]
        await_part(*final, value_part, recv_sem.at[planes * halves - 1])
        values = parts_of(*final, 0)
        for c in range(in_tile):
            value = span_rows(values, c)
            for h in range(tiles):
                weights[h * in_tile + c] = value[h : h + 1]
        for s in range(spans):
            span = order_ref[s]
            left = row_side[span] * weights[span].astype(jnp.bfloat16)
            right = column_side[span]
            full = contract_lanes(left, jnp.concatenate([right, right], axis=0))
            decoded[pl.ds(s, chunks, stride=spans), :] = partial[s] + jnp.where(lower, full[:chunks], full[chunks:])

    for k in range(chunks):
        update_ref[:, k * LANES : (k + 1) * LANES] = decoded[
            k * spans : (k + 1) * spans, :
        ].astype(jnp.bfloat16)
    for _ in range(devices - 1):
        copy_to(last, pl.ds(0, 3 * LANES), recv_sem.at[landing]).wait_send()


def store_kernel(update_ref, residual_ref, update_hbm, residual_hbm, sem):
    stores = [
        pltpu.make_async_copy(residual_ref, residual_hbm, sem.at[0]),
        pltpu.make_async_copy(update_ref, update_hbm, sem.at[1]),
    ]
    for store in stores:
        store.start()
    for store in stores:
        store.wait()


def local_small(groups, planes, momentum, picked, owner_span_order):
    spans = momentum.shape[0]
    chunks = BLOCK * BLOCK // LANES
    operands = [owner_span_order, momentum, picked]
    anywhere = pl.BlockSpec(memory_space=pl.ANY)
    vmem = pl.BlockSpec(memory_space=pltpu.VMEM)
    devices = groups * planes
    tile_shape = (spans * TOPK // LANES, 3 * LANES)
    results = pl.pallas_call(
        functools.partial(exchange_kernel, groups, planes),
        out_shape=[pltpu.VMEM(momentum.shape, jnp.bfloat16)] * 2,
        in_specs=[anywhere] * len(operands),
        out_specs=[vmem] * 2,
        scratch_shapes=[
            pltpu.SMEM(owner_span_order.shape, jnp.int32),
            pltpu.VMEM(momentum.shape, momentum.dtype),
            pltpu.VMEM(picked.shape, picked.dtype),
            pltpu.VMEM((chunks, LANES), jnp.float32),
            pltpu.VMEM((BLOCK, LANES), jnp.float32),
            pltpu.VMEM((BLOCK, LANES), jnp.bfloat16),
            pltpu.VMEM((BLOCK, BLOCK), jnp.bfloat16),
            pltpu.VMEM(tile_shape, jnp.bfloat16),
            pltpu.VMEM((devices, *tile_shape), jnp.bfloat16),
            pltpu.VMEM((spans, BLOCK, LANES), jnp.bfloat16),
            pltpu.VMEM((spans, BLOCK, BLOCK), jnp.float32),
            pltpu.VMEM((spans, chunks, LANES), jnp.float32),
            pltpu.VMEM((spans, BLOCK, LANES), jnp.bfloat16),
            pltpu.VMEM((spans, BLOCK, LANES), jnp.bfloat16),
            pltpu.VMEM((spans, 1, LANES), jnp.float32),
            pltpu.VMEM((chunks * spans, LANES), jnp.float32),
            pltpu.SemaphoreType.DMA((3,)),
            pltpu.SemaphoreType.DMA,
            pltpu.SemaphoreType.DMA((devices * TOPK // LANES,)),
            pltpu.SemaphoreType.DMA,
            pltpu.SemaphoreType.REGULAR,
        ],
        compiler_params=pltpu.CompilerParams(collective_id=0, has_side_effects=True),
    )(*operands)
    return pl.pallas_call(
        store_kernel,
        out_shape=[jax.ShapeDtypeStruct(momentum.shape, jnp.bfloat16)] * 2,
        in_specs=[vmem] * 2,
        out_specs=[anywhere] * 2,
        scratch_shapes=[pltpu.SemaphoreType.DMA((2,))],
    )(*[pltpu.with_memory_space_constraint(result, pltpu.VMEM) for result in results])


def local(groups, planes, momentum, picked, owner_span_order):
    entries = momentum.shape[0] * TOPK
    if entries % LANES == 0 and planes > 1 and groups % (LANES // TOPK) == 0 and groups * planes * entries * 8 <= GATHER_BYTES:
        return local_small(groups, planes, momentum, picked, owner_span_order)
    return local_large(momentum, picked, owner_span_order)


def solution(mesh):
    return jax.shard_map(
        functools.partial(local, mesh.shape["grp"], mesh.shape["rep"]),
        mesh=mesh,
        in_specs=(P(("grp", "rep"), None), P(("grp", "rep"), None), P()),
        out_specs=(P(), P(("grp", "rep"), None)),
        check_vma=False,
    )
```

```python
import math

import functools

import jax
import jax.numpy as jnp
from jax import lax
from jax.experimental import pallas as pl
from jax.experimental.pallas import tpu as pltpu
from jax.sharding import PartitionSpec as P

BLOCK = 64
TOPK = 32
CH_OWN = 1


def dct_cosines(points):
    freq = jnp.arange(points, dtype=jnp.float32)[:, None]
    place = jnp.arange(points, dtype=jnp.float32)[None, :]
    values = jnp.cos(jnp.pi * (2.0 * place + 1.0) * freq / (2.0 * points)) * jnp.sqrt(2.0 / points)
    values = values.at[0].multiply(jnp.sqrt(0.5))
    rounded = lax.optimization_barrier(values.astype(jnp.bfloat16))
    return rounded.astype(jnp.float32)


def forward(square_low, cosines, cos_low):
    half = jnp.einsum("cab,jb->caj", square_low, cos_low, preferred_element_type=jnp.float32)
    return jnp.einsum("ia,caj->cij", cosines, half, precision=lax.Precision.HIGHEST)


def decode(dense_matrix, cosines):
    square = dense_matrix.reshape(dense_matrix.shape[0], BLOCK, BLOCK)
    half = jnp.einsum("cij,jb->cib", square, cosines, precision=lax.Precision.HIGHEST)
    full = jnp.einsum("ia,cib->cab", cosines, half, precision=lax.Precision.HIGHEST)
    return full.reshape(dense_matrix.shape[0], BLOCK * BLOCK)


def decode_sparse(dense_low, cosines, cos_low):
    square = dense_low.reshape(dense_low.shape[0], BLOCK, BLOCK)
    half = jnp.einsum("cij,jb->cib", square, cos_low, preferred_element_type=jnp.float32)
    full = jnp.einsum("ia,cib->cab", cosines, half, precision=lax.Precision.HIGHEST)
    return full.reshape(dense_low.shape[0], BLOCK * BLOCK)


def densify(values, spots):
    entries, columns = values.shape
    per_step = math.gcd(entries, max(1, 65536 // columns))
    positions = jnp.arange(BLOCK, dtype=jnp.int32)

    def one_block(pieces):
        block_values, block_spots = pieces
        zeros = jnp.zeros_like(block_values)
        row_onehot = jnp.where(
            (block_spots // BLOCK)[:, None, :] == positions[None, :, None],
            block_values[:, None, :],
            zeros[:, None, :],
        )
        column_onehot = ((block_spots % BLOCK)[:, None, :] == positions[None, :, None]).astype(
            jnp.bfloat16
        )
        dense_matrix = jnp.einsum(
            "bcy,bzy->bcz", row_onehot, column_onehot, preferred_element_type=jnp.float32
        )
        return dense_matrix.reshape(per_step, BLOCK * BLOCK)

    stacked = lax.map(
        one_block,
        (
            values.reshape(entries // per_step, per_step, columns),
            spots.reshape(entries // per_step, per_step, columns),
        ),
    )
    return stacked.reshape(entries, BLOCK * BLOCK)


def owner_sum(received):
    values, spots = received
    return densify(values[0], spots[0])


def local_large(momentum, picked, owner_span_order):
    cosines = dct_cosines(BLOCK)
    cos_low = cosines.astype(jnp.bfloat16)
    owners = lax.axis_size("grp")
    span_count = momentum.shape[0]
    square_low = momentum.reshape(span_count, BLOCK, BLOCK)
    transform_coefficients = forward(square_low, cosines, cos_low).reshape(
        span_count, BLOCK * BLOCK
    )
    chosen = jnp.take_along_axis(transform_coefficients, picked, axis=1).astype(jnp.bfloat16)
    own_dense = densify(chosen, picked).astype(jnp.bfloat16)
    residual_momentum = (
        momentum.astype(jnp.float32) - decode_sparse(own_dense, cosines, cos_low)
    ).astype(jnp.bfloat16)
    slot_values = jnp.take(chosen, owner_span_order, axis=0)
    slot_spots = jnp.take(picked, owner_span_order, axis=0)
    shaped = (slot_values.reshape(owners, CH_OWN, TOPK), slot_spots.reshape(owners, CH_OWN, TOPK))
    partial_sum = owner_sum(
        (
            lax.all_to_all(shaped[0], "grp", split_axis=0, concat_axis=2, tiled=True),
            lax.all_to_all(shaped[1], "grp", split_axis=0, concat_axis=2, tiled=True),
        )
    )
    partial_sum = lax.psum(partial_sum, "rep")
    my_share = decode(partial_sum, cosines).astype(jnp.bfloat16)
    update = lax.all_gather(my_share, "grp", axis=0, tiled=True)
    return (update, residual_momentum)


LANES = 128
LOADS = 4
GATHER_BYTES = 2**20


def cosines_at(freq, place):
    turn = (freq * (2 * place + 1)) & (4 * BLOCK - 1)
    turn = jnp.where(turn > 2 * BLOCK, 4 * BLOCK - turn, turn)
    past = turn > BLOCK
    turn = jnp.where(past, 2 * BLOCK - turn, turn)
    angle = turn.astype(jnp.float32) * (math.pi / (2 * BLOCK))
    square = angle * angle
    value = jnp.full(square.shape, 1 / math.factorial(12), jnp.float32)
    for power in (10, 8, 6, 4, 2, 0):
        value = (-1) ** (power // 2) / math.factorial(power) + square * value
    scale = jnp.where(freq == 0, math.sqrt(1 / BLOCK), math.sqrt(2 / BLOCK))
    return (jnp.where(past, -value, value) * scale).astype(jnp.bfloat16)


def contract_lanes(left, right):
    return lax.dot_general(
        left, right, (((1,), (1,)), ((), ())), preferred_element_type=jnp.float32
    )


def matmul(left, right):
    return jnp.dot(left, right, preferred_element_type=jnp.float32)


def split(value):
    high = value.astype(jnp.bfloat16)
    return high, (value - high.astype(jnp.float32)).astype(jnp.bfloat16)


def exchange_kernel(
    groups,
    planes,
    order_hbm,
    momentum_hbm,
    picked_hbm,
    update_ref,
    residual_ref,
    order_ref,
    momentum_ref,
    picked_ref,
    rows_ref,
    wide_ref,
    twice_ref,
    pairs_ref,
    message,
    box,
    dense,
    summed,
    partial,
    row_side,
    column_side,
    weights,
    decoded,
    load_sem,
    send_sem,
    recv_sem,
    spot_sem,
    all_here,
):
    pltpu.make_async_copy(picked_hbm, picked_ref, load_sem).start()
    width = momentum_ref.shape[1] // LOADS
    for n in range(LOADS):
        piece = pl.ds(n * width, width)
        pltpu.make_async_copy(momentum_hbm.at[:, piece], momentum_ref.at[:, piece], send_sem).start()
    spans = momentum_ref.shape[0]
    entries = spans * TOPK
    chunks = BLOCK * BLOCK // LANES
    folds = chunks // 2
    in_tile = LANES // TOPK
    tiles = entries // LANES
    devices = groups * planes
    my_group, my_plane = lax.axis_index("grp"), lax.axis_index("rep")
    group_of = [lax.rem(my_group + step, groups) for step in range(groups)]
    early_planes, early_groups = max(1, planes // 2), max(1, groups // 2)
    early = early_planes * early_groups
    last = {"grp": jnp.int32(groups - 1), "rep": jnp.int32(planes - 1)}
    hubs = 2
    is_hub = jnp.logical_and(my_plane == 0, my_group < hubs)
    is_final = jnp.logical_and(my_plane == planes - 1, my_group >= groups - in_tile)
    is_last = jnp.logical_and(my_plane == planes - 1, my_group == groups - 1)
    is_early = jnp.logical_and(my_plane < early_planes, my_group < early_groups)

    def to_all(planes_of, groups_of, action):
        for z in planes_of:
            for g in groups_of:
                peer = {"grp": jnp.int32(g), "rep": jnp.int32(z)}
                is_me = jnp.logical_and(my_plane == z, my_group == g)
                pl.when(jnp.logical_not(is_me))(functools.partial(action, peer))

    def to_hubs(action):
        to_all(range(1), range(hubs), action)

    def to_others(action):
        to_all(range(1), range(hubs, early_groups), action)
        to_all(range(1, early_planes), range(early_groups), action)

    def to_early(action):
        to_hubs(action)
        to_others(action)

    def to_late(action):
        for z in range(early_planes, planes):
            for g in range(groups):
                peer = {"grp": group_of[g], "rep": jnp.int32(z)}
                if g:
                    action(peer)
                else:
                    pl.when(my_plane != z)(functools.partial(action, peer))
        to_all(range(early_planes), range(early_groups, groups), action)

    barrier = pltpu.get_barrier_semaphore()

    def signal(semaphore, peer):
        pl.semaphore_signal(semaphore, inc=1, device_id=peer, device_id_type=pl.DeviceIdType.MESH)

    @pl.when(is_early)
    def _():
        to_late(functools.partial(signal, barrier))
        to_early(functools.partial(signal, barrier))

    @pl.when(jnp.logical_not(jnp.logical_or(is_early, is_last)))
    def _():
        signal(barrier, last)

    def iotas(shape):
        return [lax.broadcasted_iota(jnp.int32, shape, d) for d in range(2)]

    line, freq = iotas((2 * folds, LANES))
    rows_ref[...] = cosines_at(freq % BLOCK, 2 * (line % folds) + line // folds).astype(jnp.float32)
    line, freq = iotas((BLOCK, BLOCK))
    pairs_ref[...] = cosines_at(freq, 2 * (line % chunks) + line // chunks)
    line, place = iotas((BLOCK, LANES))
    twice_ref[...] = cosines_at(line, place % BLOCK)
    wide_ref[...] = cosines_at(place % BLOCK, line).astype(jnp.float32)

    span, lane = iotas((spans, entries))
    turn = lax.rem(my_group, in_tile)
    block = (lane % LANES) // TOPK + in_tile - turn
    slot = lane // LANES * in_tile + jnp.where(block >= in_tile, block - in_tile, block)
    mine = span == slot

    @pl.when(is_last)
    def _():
        pl.semaphore_wait(barrier, devices - 1)
        to_late(functools.partial(signal, all_here))
        to_early(functools.partial(signal, all_here))

    pltpu.make_async_copy(picked_hbm, picked_ref, load_sem).wait()
    spread = jnp.concatenate([picked_ref[...]] * spans, axis=1)
    pltpu.make_async_copy(momentum_hbm, momentum_ref, send_sem).wait()
    spots = jnp.sum(jnp.where(mine, spread, 0), axis=0, keepdims=True)
    row_spot, col_spot = spots // BLOCK, spots % BLOCK

    def looked_up(table, spot):
        height = table.shape[0]
        return jnp.concatenate(
            [
                jnp.take_along_axis(
                    table,
                    jnp.broadcast_to(spot[:, h * LANES : (h + 1) * LANES], (height, LANES)),
                    axis=1,
                    mode="promise_in_bounds",
                )
                for h in range(tiles)
            ],
            axis=1,
        )

    odd = jnp.where(row_spot % 2 == 1, -1.0, 1.0)
    wave = looked_up(wide_ref[...], col_spot)
    mirror = (wave * odd).astype(jnp.bfloat16)
    wave = wave.astype(jnp.bfloat16)
    waves = [jnp.concatenate([wave, mirror], axis=0), jnp.concatenate([mirror, wave], axis=0)]
    half_rows = folds * spans
    row_wave = looked_up(rows_ref[...], row_spot)
    row_waves = [row_wave[p * folds : (p + 1) * folds][:, None, :] for p in range(2)]

    def by_tile(row):
        return jnp.concatenate(
            [row[:, h * LANES : (h + 1) * LANES] for h in range(tiles)], axis=0
        ).astype(jnp.bfloat16)

    me = my_plane * groups + my_group
    batches = [(planes - 2) * groups, (planes - 1) * groups, devices - in_tile, devices]
    batches = [b for b in sorted(set(batches)) if b]
    landing = sum(jnp.where(me >= b, 1, 0) for b in batches[:-1])
    value_part, spot_part = pl.ds(0, LANES), pl.ds(LANES, 2 * LANES)

    def copy_to(peer, lanes, semaphore):
        return pltpu.make_async_remote_copy(
            src_ref=message.at[:, lanes],
            dst_ref=box.at[me, :, lanes],
            send_sem=send_sem,
            recv_sem=semaphore,
            device_id=peer,
            device_id_type=pl.DeviceIdType.MESH,
        )

    def send(peer):
        copy_to(peer, pl.ds(0, 3 * LANES), recv_sem.at[landing]).start()

    def send_spots(peer):
        copy_to(peer, spot_part, spot_sem).start()

    def send_values(peer):
        copy_to(peer, value_part, recv_sem.at[landing]).start()

    message[:, LANES : 2 * LANES] = by_tile(row_spot.astype(jnp.float32))
    message[:, 2 * LANES :] = by_tile(col_spot.astype(jnp.float32))
    @pl.when(jnp.logical_and(is_final, jnp.logical_not(is_last)))
    def _():
        pl.semaphore_wait(barrier, early)

    pl.when(is_final)(lambda: to_hubs(send_spots))

    def chunk(k):
        return momentum_ref[:, k * LANES : (k + 1) * LANES].astype(jnp.float32)

    left_lanes = lax.broadcasted_iota(jnp.int32, (spans, LANES), 1) < BLOCK

    def folded(p):
        pairs = [(chunk(k), chunk(chunks - 1 - k)) for k in range(folds)]
        return jnp.concatenate([jnp.where(left_lanes, pair[p], pair[1 - p]) for pair in pairs], axis=0)

    total = jnp.zeros((spans, entries), jnp.float32)
    for p in range(2):
        product = matmul(folded(p).astype(jnp.bfloat16), waves[p]).reshape(folds, spans, entries)
        total += jnp.sum(row_waves[p] * product, axis=0)
    chosen = jnp.sum(jnp.where(mine, total, 0.0), axis=0, keepdims=True)
    message[:, :LANES] = by_tile(chosen)

    @pl.when(jnp.logical_not(is_final))
    def _():
        pl.semaphore_wait(barrier, jnp.where(is_early, early - 1, early))
        to_hubs(send)

    pl.when(is_final)(lambda: to_hubs(send_values))
    to_others(send)

    pltpu.make_async_copy(message, box.at[me], recv_sem.at[landing]).start()

    pltpu.make_async_copy(order_hbm, order_ref, load_sem).start()
    chosen = chosen.astype(jnp.bfloat16).astype(jnp.float32)
    scaled = jnp.where(mine, chosen, 0.0)
    residuals = []
    for p in range(2):
        weight = row_waves[p] * scaled[None]
        residual = folded(p)
        for part in split(weight.reshape(half_rows, entries)):
            residual -= contract_lanes(part, waves[p])
        residuals.append(residual)
    for k in range(folds):
        pair = [residual[k * spans : (k + 1) * spans] for residual in residuals]
        for n, at in enumerate((k, chunks - 1 - k)):
            residual_ref[:, at * LANES : (at + 1) * LANES] = jnp.where(
                left_lanes, pair[n], pair[1 - n]
            ).astype(jnp.bfloat16)

    @pl.when(jnp.logical_not(is_last))
    def _():
        pl.semaphore_wait(all_here, 1)

    to_late(send)

    block = lax.broadcasted_iota(jnp.int32, (tiles, LANES), 1) // TOPK
    taken = [block == turn for turn in range(in_tile)]
    one, zero = jnp.ones((), jnp.bfloat16), jnp.zeros((), jnp.bfloat16)

    def await_part(n, lanes, semaphore):
        start = batches[n - 1] if n else 0
        landed = box.at[pl.ds(start, batches[n] - start), :, lanes]
        pltpu.make_async_copy(landed, landed, semaphore).wait()

    def parts_of(first, part):
        lanes = slice(part * LANES, (part + 1) * LANES)
        return [box[first + n, :, lanes].astype(jnp.float32) for n in range(in_tile)]

    def span_rows(parts, c):
        row = parts[0]
        for turn in range(1, in_tile):
            row = jnp.where(taken[(c + turn) % in_tile], parts[turn], row)
        return row

    def spread_out(row, freq, fill):
        return jnp.where(freq == row, fill, zero)

    def add_up(n, sums):
        await_part(n, pl.ds(0, 3 * LANES), recv_sem.at[n])
        firsts = list(range(batches[n - 1] if n else 0, batches[n], in_tile))
        for group in (firsts[m : m + 2] for m in range(0, len(firsts), 2)):
            pieces = [[parts_of(first, part) for part in range(3)] for first in group]
            freq = lax.broadcasted_iota(jnp.int32, (BLOCK, len(group) * LANES), 0)
            freq = freq.astype(jnp.float32).astype(jnp.bfloat16)
            for c in range(in_tile):
                value, row, column = (
                    jnp.concatenate([span_rows(piece[n], c) for piece in pieces], axis=1).astype(jnp.bfloat16)
                    for n in range(3)
                )
                for h in range(tiles):
                    left = spread_out(row[h : h + 1], freq, one)
                    right = spread_out(column[h : h + 1], freq, value[h : h + 1])
                    part = contract_lanes(left, right)
                    s = h * in_tile + c
                    sums[s] = part if sums[s] is None else sums[s] + part
        return sums

    lower = lax.broadcasted_iota(jnp.int32, (chunks, LANES), 1) < BLOCK

    def slot_matrices(sums):
        for s in range(spans):
            dense[s] = matmul(sums[s].astype(jnp.bfloat16), twice_ref[...]).astype(jnp.bfloat16)
        for s in range(spans):
            full = matmul(pairs_ref[...], dense[order_ref[s]])
            yield s, jnp.where(lower, full[:chunks], full[chunks:])

    sums = [None] * spans
    for n in range(len(batches) - 1):
        sums = add_up(n, sums)
    for s in range(spans):
        summed[s] = sums[s]
    pltpu.make_async_copy(order_hbm, order_ref, load_sem).wait()

    @pl.when(jnp.logical_not(is_hub))
    def _():
        for s, matrix in slot_matrices(add_up(len(batches) - 1, [summed[s] for s in range(spans)])):
            decoded[pl.ds(s, chunks, stride=spans), :] = matrix

    @pl.when(is_hub)
    def _():
        for s, matrix in slot_matrices([summed[s] for s in range(spans)]):
            partial[s] = matrix
        await_part(len(batches) - 1, spot_part, spot_sem)
        freq = lax.broadcasted_iota(jnp.int32, (BLOCK, entries), 0)
        freq = freq.astype(jnp.float32).astype(jnp.bfloat16)
        rows, columns = (parts_of(devices - in_tile, part) for part in (1, 2))
        for c in range(in_tile):
            row, column = (
                jnp.concatenate([span_rows(parts, c)[h : h + 1] for h in range(tiles)], axis=1).astype(jnp.bfloat16)
                for parts in (rows, columns)
            )
            left = matmul(pairs_ref[...], spread_out(row, freq, one)).astype(jnp.bfloat16)
            right = matmul(wide_ref[:, :BLOCK].astype(jnp.bfloat16), spread_out(column, freq, one)).astype(jnp.bfloat16)
            for h in range(tiles):
                row_side[h * in_tile + c] = left[:, h * LANES : (h + 1) * LANES]
                column_side[h * in_tile + c] = right[:, h * LANES : (h + 1) * LANES]
        await_part(len(batches) - 1, value_part, recv_sem.at[len(batches) - 1])
        values = parts_of(devices - in_tile, 0)
        for c in range(in_tile):
            value = span_rows(values, c)
            for h in range(tiles):
                weights[h * in_tile + c] = value[h : h + 1]
        for s in range(spans):
            span = order_ref[s]
            left = row_side[span] * weights[span].astype(jnp.bfloat16)
            right = column_side[span]
            full = contract_lanes(left, jnp.concatenate([right, right], axis=0))
            decoded[pl.ds(s, chunks, stride=spans), :] = partial[s] + jnp.where(lower, full[:chunks], full[chunks:])

    for k in range(chunks):
        update_ref[:, k * LANES : (k + 1) * LANES] = decoded[
            k * spans : (k + 1) * spans, :
        ].astype(jnp.bfloat16)
    for _ in range(devices - 1):
        copy_to(last, pl.ds(0, 3 * LANES), recv_sem.at[landing]).wait_send()


def store_kernel(update_ref, residual_ref, update_hbm, residual_hbm, sem):
    stores = [
        pltpu.make_async_copy(residual_ref, residual_hbm, sem.at[0]),
        pltpu.make_async_copy(update_ref, update_hbm, sem.at[1]),
    ]
    for store in stores:
        store.start()
    for store in stores:
        store.wait()


def local_small(groups, planes, momentum, picked, owner_span_order):
    spans = momentum.shape[0]
    chunks = BLOCK * BLOCK // LANES
    operands = [owner_span_order, momentum, picked]
    anywhere = pl.BlockSpec(memory_space=pl.ANY)
    vmem = pl.BlockSpec(memory_space=pltpu.VMEM)
    devices = groups * planes
    tile_shape = (spans * TOPK // LANES, 3 * LANES)
    results = pl.pallas_call(
        functools.partial(exchange_kernel, groups, planes),
        out_shape=[pltpu.VMEM(momentum.shape, jnp.bfloat16)] * 2,
        in_specs=[anywhere] * len(operands),
        out_specs=[vmem] * 2,
        scratch_shapes=[
            pltpu.SMEM(owner_span_order.shape, jnp.int32),
            pltpu.VMEM(momentum.shape, momentum.dtype),
            pltpu.VMEM(picked.shape, picked.dtype),
            pltpu.VMEM((chunks, LANES), jnp.float32),
            pltpu.VMEM((BLOCK, LANES), jnp.float32),
            pltpu.VMEM((BLOCK, LANES), jnp.bfloat16),
            pltpu.VMEM((BLOCK, BLOCK), jnp.bfloat16),
            pltpu.VMEM(tile_shape, jnp.bfloat16),
            pltpu.VMEM((devices, *tile_shape), jnp.bfloat16),
            pltpu.VMEM((spans, BLOCK, LANES), jnp.bfloat16),
            pltpu.VMEM((spans, BLOCK, BLOCK), jnp.float32),
            pltpu.VMEM((spans, chunks, LANES), jnp.float32),
            pltpu.VMEM((spans, BLOCK, LANES), jnp.bfloat16),
            pltpu.VMEM((spans, BLOCK, LANES), jnp.bfloat16),
            pltpu.VMEM((spans, 1, LANES), jnp.float32),
            pltpu.VMEM((chunks * spans, LANES), jnp.float32),
            pltpu.SemaphoreType.DMA,
            pltpu.SemaphoreType.DMA,
            pltpu.SemaphoreType.DMA((4,)),
            pltpu.SemaphoreType.DMA,
            pltpu.SemaphoreType.REGULAR,
        ],
        compiler_params=pltpu.CompilerParams(collective_id=0, has_side_effects=True),
    )(*operands)
    return pl.pallas_call(
        store_kernel,
        out_shape=[jax.ShapeDtypeStruct(momentum.shape, jnp.bfloat16)] * 2,
        in_specs=[vmem] * 2,
        out_specs=[anywhere] * 2,
        scratch_shapes=[pltpu.SemaphoreType.DMA((2,))],
    )(*[pltpu.with_memory_space_constraint(result, pltpu.VMEM) for result in results])


def local(groups, planes, momentum, picked, owner_span_order):
    entries = momentum.shape[0] * TOPK
    if entries % LANES == 0 and planes > 1 and groups > LANES // TOPK and groups % (LANES // TOPK) == 0 and groups * planes * entries * 8 <= GATHER_BYTES:
        return local_small(groups, planes, momentum, picked, owner_span_order)
    return local_large(momentum, picked, owner_span_order)


def solution(mesh):
    return jax.shard_map(
        functools.partial(local, mesh.shape["grp"], mesh.shape["rep"]),
        mesh=mesh,
        in_specs=(P(("grp", "rep"), None), P(("grp", "rep"), None), P()),
        out_specs=(P(), P(("grp", "rep"), None)),
        check_vma=False,
    )
```

```python
import math

import functools

import jax
import jax.numpy as jnp
from jax import lax
from jax.experimental import pallas as pl
from jax.experimental.pallas import tpu as pltpu
from jax.sharding import PartitionSpec as P

BLOCK = 64
TOPK = 32
CH_OWN = 1


def dct_cosines(points):
    freq = jnp.arange(points, dtype=jnp.float32)[:, None]
    place = jnp.arange(points, dtype=jnp.float32)[None, :]
    values = jnp.cos(jnp.pi * (2.0 * place + 1.0) * freq / (2.0 * points)) * jnp.sqrt(2.0 / points)
    values = values.at[0].multiply(jnp.sqrt(0.5))
    rounded = lax.optimization_barrier(values.astype(jnp.bfloat16))
    return rounded.astype(jnp.float32)


def forward(square_low, cosines, cos_low):
    half = jnp.einsum("cab,jb->caj", square_low, cos_low, preferred_element_type=jnp.float32)
    return jnp.einsum("ia,caj->cij", cosines, half, precision=lax.Precision.HIGHEST)


def decode(dense_matrix, cosines):
    square = dense_matrix.reshape(dense_matrix.shape[0], BLOCK, BLOCK)
    half = jnp.einsum("cij,jb->cib", square, cosines, precision=lax.Precision.HIGHEST)
    full = jnp.einsum("ia,cib->cab", cosines, half, precision=lax.Precision.HIGHEST)
    return full.reshape(dense_matrix.shape[0], BLOCK * BLOCK)


def decode_sparse(dense_low, cosines, cos_low):
    square = dense_low.reshape(dense_low.shape[0], BLOCK, BLOCK)
    half = jnp.einsum("cij,jb->cib", square, cos_low, preferred_element_type=jnp.float32)
    full = jnp.einsum("ia,cib->cab", cosines, half, precision=lax.Precision.HIGHEST)
    return full.reshape(dense_low.shape[0], BLOCK * BLOCK)


def densify(values, spots):
    entries, columns = values.shape
    per_step = math.gcd(entries, max(1, 65536 // columns))
    positions = jnp.arange(BLOCK, dtype=jnp.int32)

    def one_block(pieces):
        block_values, block_spots = pieces
        zeros = jnp.zeros_like(block_values)
        row_onehot = jnp.where(
            (block_spots // BLOCK)[:, None, :] == positions[None, :, None],
            block_values[:, None, :],
            zeros[:, None, :],
        )
        column_onehot = ((block_spots % BLOCK)[:, None, :] == positions[None, :, None]).astype(
            jnp.bfloat16
        )
        dense_matrix = jnp.einsum(
            "bcy,bzy->bcz", row_onehot, column_onehot, preferred_element_type=jnp.float32
        )
        return dense_matrix.reshape(per_step, BLOCK * BLOCK)

    stacked = lax.map(
        one_block,
        (
            values.reshape(entries // per_step, per_step, columns),
            spots.reshape(entries // per_step, per_step, columns),
        ),
    )
    return stacked.reshape(entries, BLOCK * BLOCK)


def owner_sum(received):
    values, spots = received
    return densify(values[0], spots[0])


def local_large(momentum, picked, owner_span_order):
    cosines = dct_cosines(BLOCK)
    cos_low = cosines.astype(jnp.bfloat16)
    owners = lax.axis_size("grp")
    span_count = momentum.shape[0]
    square_low = momentum.reshape(span_count, BLOCK, BLOCK)
    transform_coefficients = forward(square_low, cosines, cos_low).reshape(
        span_count, BLOCK * BLOCK
    )
    chosen = jnp.take_along_axis(transform_coefficients, picked, axis=1).astype(jnp.bfloat16)
    own_dense = densify(chosen, picked).astype(jnp.bfloat16)
    residual_momentum = (
        momentum.astype(jnp.float32) - decode_sparse(own_dense, cosines, cos_low)
    ).astype(jnp.bfloat16)
    slot_values = jnp.take(chosen, owner_span_order, axis=0)
    slot_spots = jnp.take(picked, owner_span_order, axis=0)
    shaped = (slot_values.reshape(owners, CH_OWN, TOPK), slot_spots.reshape(owners, CH_OWN, TOPK))
    partial_sum = owner_sum(
        (
            lax.all_to_all(shaped[0], "grp", split_axis=0, concat_axis=2, tiled=True),
            lax.all_to_all(shaped[1], "grp", split_axis=0, concat_axis=2, tiled=True),
        )
    )
    partial_sum = lax.psum(partial_sum, "rep")
    my_share = decode(partial_sum, cosines).astype(jnp.bfloat16)
    update = lax.all_gather(my_share, "grp", axis=0, tiled=True)
    return (update, residual_momentum)


LANES = 128
LOADS = 4
GATHER_BYTES = 2**20


def cosines_at(freq, place):
    turn = (freq * (2 * place + 1)) & (4 * BLOCK - 1)
    turn = jnp.where(turn > 2 * BLOCK, 4 * BLOCK - turn, turn)
    past = turn > BLOCK
    turn = jnp.where(past, 2 * BLOCK - turn, turn)
    angle = turn.astype(jnp.float32) * (math.pi / (2 * BLOCK))
    square = angle * angle
    value = jnp.full(square.shape, 1 / math.factorial(12), jnp.float32)
    for power in (10, 8, 6, 4, 2, 0):
        value = (-1) ** (power // 2) / math.factorial(power) + square * value
    scale = jnp.where(freq == 0, math.sqrt(1 / BLOCK), math.sqrt(2 / BLOCK))
    return (jnp.where(past, -value, value) * scale).astype(jnp.bfloat16)


def contract_lanes(left, right):
    return lax.dot_general(
        left, right, (((1,), (1,)), ((), ())), preferred_element_type=jnp.float32
    )


def matmul(left, right):
    return jnp.dot(left, right, preferred_element_type=jnp.float32)


def split(value):
    high = value.astype(jnp.bfloat16)
    return high, (value - high.astype(jnp.float32)).astype(jnp.bfloat16)


def exchange_kernel(
    groups,
    planes,
    order_hbm,
    momentum_hbm,
    picked_hbm,
    update_ref,
    residual_ref,
    order_ref,
    momentum_ref,
    picked_ref,
    rows_ref,
    wide_ref,
    twice_ref,
    pairs_ref,
    message,
    box,
    dense,
    summed,
    partial,
    row_side,
    column_side,
    weights,
    decoded,
    load_sem,
    send_sem,
    recv_sem,
    spot_sem,
    all_here,
):
    pltpu.make_async_copy(picked_hbm, picked_ref, load_sem).start()
    width = momentum_ref.shape[1] // LOADS
    for n in range(LOADS):
        piece = pl.ds(n * width, width)
        pltpu.make_async_copy(momentum_hbm.at[:, piece], momentum_ref.at[:, piece], send_sem).start()
    spans = momentum_ref.shape[0]
    entries = spans * TOPK
    chunks = BLOCK * BLOCK // LANES
    folds = chunks // 2
    in_tile = LANES // TOPK
    tiles = entries // LANES
    devices = groups * planes
    my_group, my_plane = lax.axis_index("grp"), lax.axis_index("rep")
    group_of = [lax.rem(my_group + step, groups) for step in range(groups)]
    early_planes, early_groups = max(1, planes // 2), max(1, groups // 2)
    early = early_planes * early_groups
    last = {"grp": jnp.int32(groups - 1), "rep": jnp.int32(planes - 1)}
    hubs = 2
    is_hub = jnp.logical_and(my_plane == 0, my_group < hubs)
    is_final = jnp.logical_and(my_plane == planes - 1, my_group >= groups - in_tile)
    is_last = jnp.logical_and(my_plane == planes - 1, my_group == groups - 1)
    is_early = jnp.logical_and(my_plane < early_planes, my_group < early_groups)

    def to_all(planes_of, groups_of, action):
        for z in planes_of:
            for g in groups_of:
                peer = {"grp": jnp.int32(g), "rep": jnp.int32(z)}
                is_me = jnp.logical_and(my_plane == z, my_group == g)
                pl.when(jnp.logical_not(is_me))(functools.partial(action, peer))

    def to_hubs(action):
        to_all(range(1), range(hubs), action)

    def to_others(action):
        to_all(range(1), range(hubs, early_groups), action)
        to_all(range(1, early_planes), range(early_groups), action)

    def to_early(action):
        to_hubs(action)
        to_others(action)

    def to_late(action):
        for z in range(early_planes, planes):
            for g in range(groups):
                peer = {"grp": group_of[g], "rep": jnp.int32(z)}
                if g:
                    action(peer)
                else:
                    pl.when(my_plane != z)(functools.partial(action, peer))
        to_all(range(early_planes), range(early_groups, groups), action)

    barrier = pltpu.get_barrier_semaphore()

    def signal(semaphore, peer):
        pl.semaphore_signal(semaphore, inc=1, device_id=peer, device_id_type=pl.DeviceIdType.MESH)

    @pl.when(is_early)
    def _():
        to_late(functools.partial(signal, barrier))
        to_early(functools.partial(signal, barrier))

    @pl.when(jnp.logical_not(jnp.logical_or(is_early, is_last)))
    def _():
        signal(barrier, last)

    def iotas(shape):
        return [lax.broadcasted_iota(jnp.int32, shape, d) for d in range(2)]

    line, freq = iotas((2 * folds, LANES))
    rows_ref[...] = cosines_at(freq % BLOCK, 2 * (line % folds) + line // folds).astype(jnp.float32)
    line, freq = iotas((BLOCK, BLOCK))
    pairs_ref[...] = cosines_at(freq, 2 * (line % chunks) + line // chunks)
    line, place = iotas((BLOCK, LANES))
    twice_ref[...] = cosines_at(line, place % BLOCK)
    wide_ref[...] = cosines_at(place % BLOCK, line).astype(jnp.float32)

    span, lane = iotas((spans, entries))
    turn = lax.rem(my_group, in_tile)
    block = (lane % LANES) // TOPK + in_tile - turn
    slot = lane // LANES * in_tile + jnp.where(block >= in_tile, block - in_tile, block)
    mine = span == slot

    @pl.when(is_last)
    def _():
        pl.semaphore_wait(barrier, devices - 1)
        to_late(functools.partial(signal, all_here))
        to_early(functools.partial(signal, all_here))

    pltpu.make_async_copy(picked_hbm, picked_ref, load_sem).wait()
    spread = jnp.concatenate([picked_ref[...]] * spans, axis=1)
    pltpu.make_async_copy(momentum_hbm, momentum_ref, send_sem).wait()
    spots = jnp.sum(jnp.where(mine, spread, 0), axis=0, keepdims=True)
    row_spot, col_spot = spots // BLOCK, spots % BLOCK

    def by_tile(row):
        return jnp.concatenate(
            [row[:, h * LANES : (h + 1) * LANES] for h in range(tiles)], axis=0
        ).astype(jnp.bfloat16)

    me = my_plane * groups + my_group
    batches = [(planes - 2) * groups, (planes - 1) * groups, devices - in_tile, devices]
    batches = [b for b in sorted(set(batches)) if b]
    landing = sum(jnp.where(me >= b, 1, 0) for b in batches[:-1])
    value_part, spot_part = pl.ds(0, LANES), pl.ds(LANES, 2 * LANES)

    def copy_to(peer, lanes, semaphore):
        return pltpu.make_async_remote_copy(
            src_ref=message.at[:, lanes],
            dst_ref=box.at[me, :, lanes],
            send_sem=send_sem,
            recv_sem=semaphore,
            device_id=peer,
            device_id_type=pl.DeviceIdType.MESH,
        )

    def send(peer):
        copy_to(peer, pl.ds(0, 3 * LANES), recv_sem.at[landing]).start()

    def send_spots(peer):
        copy_to(peer, spot_part, spot_sem).start()

    def send_values(peer):
        copy_to(peer, value_part, recv_sem.at[landing]).start()

    message[:, LANES : 2 * LANES] = by_tile(row_spot.astype(jnp.float32))
    message[:, 2 * LANES :] = by_tile(col_spot.astype(jnp.float32))
    @pl.when(jnp.logical_and(is_final, jnp.logical_not(is_last)))
    def _():
        pl.semaphore_wait(barrier, early)

    pl.when(is_final)(lambda: to_hubs(send_spots))

    def looked_up(table, spot):
        height = table.shape[0]
        return jnp.concatenate(
            [
                jnp.take_along_axis(
                    table,
                    jnp.broadcast_to(spot[:, h * LANES : (h + 1) * LANES], (height, LANES)),
                    axis=1,
                    mode="promise_in_bounds",
                )
                for h in range(tiles)
            ],
            axis=1,
        )

    odd = jnp.where(row_spot % 2 == 1, -1.0, 1.0)
    wave = looked_up(wide_ref[...], col_spot)
    mirror = (wave * odd).astype(jnp.bfloat16)
    wave = wave.astype(jnp.bfloat16)
    waves = [jnp.concatenate([wave, mirror], axis=0), jnp.concatenate([mirror, wave], axis=0)]
    half_rows = folds * spans
    row_wave = looked_up(rows_ref[...], row_spot)
    row_waves = [row_wave[p * folds : (p + 1) * folds][:, None, :] for p in range(2)]


    def chunk(k):
        return momentum_ref[:, k * LANES : (k + 1) * LANES].astype(jnp.float32)

    left_lanes = lax.broadcasted_iota(jnp.int32, (spans, LANES), 1) < BLOCK

    def folded(p):
        pairs = [(chunk(k), chunk(chunks - 1 - k)) for k in range(folds)]
        return jnp.concatenate([jnp.where(left_lanes, pair[p], pair[1 - p]) for pair in pairs], axis=0)

    total = jnp.zeros((spans, entries), jnp.float32)
    for p in range(2):
        product = matmul(folded(p).astype(jnp.bfloat16), waves[p]).reshape(folds, spans, entries)
        total += jnp.sum(row_waves[p] * product, axis=0)
    chosen = jnp.sum(jnp.where(mine, total, 0.0), axis=0, keepdims=True)
    message[:, :LANES] = by_tile(chosen)

    @pl.when(jnp.logical_not(is_final))
    def _():
        pl.semaphore_wait(barrier, jnp.where(is_early, early - 1, early))
        to_hubs(send)

    pl.when(is_final)(lambda: to_hubs(send_values))
    to_others(send)

    pltpu.make_async_copy(message, box.at[me], recv_sem.at[landing]).start()

    pltpu.make_async_copy(order_hbm, order_ref, load_sem).start()
    chosen = chosen.astype(jnp.bfloat16).astype(jnp.float32)
    scaled = jnp.where(mine, chosen, 0.0)
    residuals = []
    for p in range(2):
        weight = row_waves[p] * scaled[None]
        residual = folded(p)
        for part in split(weight.reshape(half_rows, entries)):
            residual -= contract_lanes(part, waves[p])
        residuals.append(residual)
    for k in range(folds):
        pair = [residual[k * spans : (k + 1) * spans] for residual in residuals]
        for n, at in enumerate((k, chunks - 1 - k)):
            residual_ref[:, at * LANES : (at + 1) * LANES] = jnp.where(
                left_lanes, pair[n], pair[1 - n]
            ).astype(jnp.bfloat16)

    @pl.when(jnp.logical_not(is_last))
    def _():
        pl.semaphore_wait(all_here, 1)

    to_late(send)

    block = lax.broadcasted_iota(jnp.int32, (tiles, LANES), 1) // TOPK
    taken = [block == turn for turn in range(in_tile)]
    one, zero = jnp.ones((), jnp.bfloat16), jnp.zeros((), jnp.bfloat16)

    def await_part(n, lanes, semaphore):
        start = batches[n - 1] if n else 0
        landed = box.at[pl.ds(start, batches[n] - start), :, lanes]
        pltpu.make_async_copy(landed, landed, semaphore).wait()

    def parts_of(first, part):
        lanes = slice(part * LANES, (part + 1) * LANES)
        return [box[first + n, :, lanes].astype(jnp.float32) for n in range(in_tile)]

    def span_rows(parts, c):
        row = parts[0]
        for turn in range(1, in_tile):
            row = jnp.where(taken[(c + turn) % in_tile], parts[turn], row)
        return row

    def spread_out(row, freq, fill):
        return jnp.where(freq == row, fill, zero)

    def add_up(n, sums):
        await_part(n, pl.ds(0, 3 * LANES), recv_sem.at[n])
        firsts = list(range(batches[n - 1] if n else 0, batches[n], in_tile))
        for group in (firsts[m : m + 2] for m in range(0, len(firsts), 2)):
            pieces = [[parts_of(first, part) for part in range(3)] for first in group]
            freq = lax.broadcasted_iota(jnp.int32, (BLOCK, len(group) * LANES), 0)
            freq = freq.astype(jnp.float32).astype(jnp.bfloat16)
            for c in range(in_tile):
                value, row, column = (
                    jnp.concatenate([span_rows(piece[n], c) for piece in pieces], axis=1).astype(jnp.bfloat16)
                    for n in range(3)
                )
                for h in range(tiles):
                    left = spread_out(row[h : h + 1], freq, one)
                    right = spread_out(column[h : h + 1], freq, value[h : h + 1])
                    part = contract_lanes(left, right)
                    s = h * in_tile + c
                    sums[s] = part if sums[s] is None else sums[s] + part
        return sums

    lower = lax.broadcasted_iota(jnp.int32, (chunks, LANES), 1) < BLOCK

    def slot_matrices(sums):
        for s in range(spans):
            dense[s] = matmul(sums[s].astype(jnp.bfloat16), twice_ref[...]).astype(jnp.bfloat16)
        for s in range(spans):
            full = matmul(pairs_ref[...], dense[order_ref[s]])
            yield s, jnp.where(lower, full[:chunks], full[chunks:])

    sums = [None] * spans
    for n in range(len(batches) - 1):
        sums = add_up(n, sums)
    for s in range(spans):
        summed[s] = sums[s]
    pltpu.make_async_copy(order_hbm, order_ref, load_sem).wait()

    @pl.when(jnp.logical_not(is_hub))
    def _():
        for s, matrix in slot_matrices(add_up(len(batches) - 1, [summed[s] for s in range(spans)])):
            decoded[pl.ds(s, chunks, stride=spans), :] = matrix

    @pl.when(is_hub)
    def _():
        for s, matrix in slot_matrices([summed[s] for s in range(spans)]):
            partial[s] = matrix
        await_part(len(batches) - 1, spot_part, spot_sem)
        freq = lax.broadcasted_iota(jnp.int32, (BLOCK, entries), 0)
        freq = freq.astype(jnp.float32).astype(jnp.bfloat16)
        rows, columns = (parts_of(devices - in_tile, part) for part in (1, 2))
        for c in range(in_tile):
            row, column = (
                jnp.concatenate([span_rows(parts, c)[h : h + 1] for h in range(tiles)], axis=1).astype(jnp.bfloat16)
                for parts in (rows, columns)
            )
            left = matmul(pairs_ref[...], spread_out(row, freq, one)).astype(jnp.bfloat16)
            right = matmul(wide_ref[:, :BLOCK].astype(jnp.bfloat16), spread_out(column, freq, one)).astype(jnp.bfloat16)
            for h in range(tiles):
                row_side[h * in_tile + c] = left[:, h * LANES : (h + 1) * LANES]
                column_side[h * in_tile + c] = right[:, h * LANES : (h + 1) * LANES]
        await_part(len(batches) - 1, value_part, recv_sem.at[len(batches) - 1])
        values = parts_of(devices - in_tile, 0)
        for c in range(in_tile):
            value = span_rows(values, c)
            for h in range(tiles):
                weights[h * in_tile + c] = value[h : h + 1]
        for s in range(spans):
            span = order_ref[s]
            left = row_side[span] * jnp.broadcast_to(weights[span], (BLOCK, LANES)).astype(jnp.bfloat16)
            right = column_side[span]
            full = contract_lanes(left, jnp.concatenate([right, right], axis=0))
            decoded[pl.ds(s, chunks, stride=spans), :] = partial[s] + jnp.where(lower, full[:chunks], full[chunks:])

    for k in range(chunks):
        update_ref[:, k * LANES : (k + 1) * LANES] = decoded[
            k * spans : (k + 1) * spans, :
        ].astype(jnp.bfloat16)
    for _ in range(devices - 1):
        copy_to(last, pl.ds(0, 3 * LANES), recv_sem.at[landing]).wait_send()


def store_kernel(update_ref, residual_ref, update_hbm, residual_hbm, both, sem):
    pltpu.make_async_copy(residual_ref, residual_hbm, sem).start()
    pltpu.make_async_copy(update_ref, update_hbm, sem).start()
    pltpu.make_async_copy(both, both, sem).wait()


def local_small(groups, planes, momentum, picked, owner_span_order):
    spans = momentum.shape[0]
    chunks = BLOCK * BLOCK // LANES
    operands = [owner_span_order, momentum, picked]
    anywhere = pl.BlockSpec(memory_space=pl.ANY)
    vmem = pl.BlockSpec(memory_space=pltpu.VMEM)
    devices = groups * planes
    tile_shape = (spans * TOPK // LANES, 3 * LANES)
    results = pl.pallas_call(
        functools.partial(exchange_kernel, groups, planes),
        out_shape=[pltpu.VMEM(momentum.shape, jnp.bfloat16)] * 2,
        in_specs=[anywhere] * len(operands),
        out_specs=[vmem] * 2,
        scratch_shapes=[
            pltpu.SMEM(owner_span_order.shape, jnp.int32),
            pltpu.VMEM(momentum.shape, momentum.dtype),
            pltpu.VMEM(picked.shape, picked.dtype),
            pltpu.VMEM((chunks, LANES), jnp.float32),
            pltpu.VMEM((BLOCK, LANES), jnp.float32),
            pltpu.VMEM((BLOCK, LANES), jnp.bfloat16),
            pltpu.VMEM((BLOCK, BLOCK), jnp.bfloat16),
            pltpu.VMEM(tile_shape, jnp.bfloat16),
            pltpu.VMEM((devices, *tile_shape), jnp.bfloat16),
            pltpu.VMEM((spans, BLOCK, LANES), jnp.bfloat16),
            pltpu.VMEM((spans, BLOCK, BLOCK), jnp.float32),
            pltpu.VMEM((spans, chunks, LANES), jnp.float32),
            pltpu.VMEM((spans, BLOCK, LANES), jnp.bfloat16),
            pltpu.VMEM((spans, BLOCK, LANES), jnp.bfloat16),
            pltpu.VMEM((spans, 1, LANES), jnp.float32),
            pltpu.VMEM((chunks * spans, LANES), jnp.float32),
            pltpu.SemaphoreType.DMA,
            pltpu.SemaphoreType.DMA,
            pltpu.SemaphoreType.DMA((4,)),
            pltpu.SemaphoreType.DMA,
            pltpu.SemaphoreType.REGULAR,
        ],
        compiler_params=pltpu.CompilerParams(collective_id=0, has_side_effects=True),
    )(*operands)
    return pl.pallas_call(
        store_kernel,
        out_shape=[jax.ShapeDtypeStruct(momentum.shape, jnp.bfloat16)] * 2,
        in_specs=[vmem] * 2,
        out_specs=[anywhere] * 2,
        scratch_shapes=[pltpu.VMEM((2, *momentum.shape), jnp.bfloat16), pltpu.SemaphoreType.DMA],
    )(*[pltpu.with_memory_space_constraint(result, pltpu.VMEM) for result in results])


def local(groups, planes, momentum, picked, owner_span_order):
    entries = momentum.shape[0] * TOPK
    if entries % LANES == 0 and planes > 1 and groups > LANES // TOPK and groups % (LANES // TOPK) == 0 and groups * planes * entries * 8 <= GATHER_BYTES:
        return local_small(groups, planes, momentum, picked, owner_span_order)
    return local_large(momentum, picked, owner_span_order)


def solution(mesh):
    return jax.shard_map(
        functools.partial(local, mesh.shape["grp"], mesh.shape["rep"]),
        mesh=mesh,
        in_specs=(P(("grp", "rep"), None), P(("grp", "rep"), None), P()),
        out_specs=(P(), P(("grp", "rep"), None)),
        check_vma=False,
    )
```

```python
import math

import functools

import jax
import jax.numpy as jnp
from jax import lax
from jax.experimental import pallas as pl
from jax.experimental.pallas import tpu as pltpu
from jax.sharding import PartitionSpec as P

BLOCK = 64
TOPK = 32
CH_OWN = 1


def dct_cosines(points):
    freq = jnp.arange(points, dtype=jnp.float32)[:, None]
    place = jnp.arange(points, dtype=jnp.float32)[None, :]
    values = jnp.cos(jnp.pi * (2.0 * place + 1.0) * freq / (2.0 * points)) * jnp.sqrt(2.0 / points)
    values = values.at[0].multiply(jnp.sqrt(0.5))
    rounded = lax.optimization_barrier(values.astype(jnp.bfloat16))
    return rounded.astype(jnp.float32)


def forward(square_low, cosines, cos_low):
    half = jnp.einsum("cab,jb->caj", square_low, cos_low, preferred_element_type=jnp.float32)
    return jnp.einsum("ia,caj->cij", cosines, half, precision=lax.Precision.HIGHEST)


def decode(dense_matrix, cosines):
    square = dense_matrix.reshape(dense_matrix.shape[0], BLOCK, BLOCK)
    half = jnp.einsum("cij,jb->cib", square, cosines, precision=lax.Precision.HIGHEST)
    full = jnp.einsum("ia,cib->cab", cosines, half, precision=lax.Precision.HIGHEST)
    return full.reshape(dense_matrix.shape[0], BLOCK * BLOCK)


def decode_sparse(dense_low, cosines, cos_low):
    square = dense_low.reshape(dense_low.shape[0], BLOCK, BLOCK)
    half = jnp.einsum("cij,jb->cib", square, cos_low, preferred_element_type=jnp.float32)
    full = jnp.einsum("ia,cib->cab", cosines, half, precision=lax.Precision.HIGHEST)
    return full.reshape(dense_low.shape[0], BLOCK * BLOCK)


def densify(values, spots):
    entries, columns = values.shape
    per_step = math.gcd(entries, max(1, 65536 // columns))
    positions = jnp.arange(BLOCK, dtype=jnp.int32)

    def one_block(pieces):
        block_values, block_spots = pieces
        zeros = jnp.zeros_like(block_values)
        row_onehot = jnp.where(
            (block_spots // BLOCK)[:, None, :] == positions[None, :, None],
            block_values[:, None, :],
            zeros[:, None, :],
        )
        column_onehot = ((block_spots % BLOCK)[:, None, :] == positions[None, :, None]).astype(
            jnp.bfloat16
        )
        dense_matrix = jnp.einsum(
            "bcy,bzy->bcz", row_onehot, column_onehot, preferred_element_type=jnp.float32
        )
        return dense_matrix.reshape(per_step, BLOCK * BLOCK)

    stacked = lax.map(
        one_block,
        (
            values.reshape(entries // per_step, per_step, columns),
            spots.reshape(entries // per_step, per_step, columns),
        ),
    )
    return stacked.reshape(entries, BLOCK * BLOCK)


def owner_sum(received):
    values, spots = received
    return densify(values[0], spots[0])


def local_large(momentum, picked, owner_span_order):
    cosines = dct_cosines(BLOCK)
    cos_low = cosines.astype(jnp.bfloat16)
    owners = lax.axis_size("grp")
    span_count = momentum.shape[0]
    square_low = momentum.reshape(span_count, BLOCK, BLOCK)
    transform_coefficients = forward(square_low, cosines, cos_low).reshape(
        span_count, BLOCK * BLOCK
    )
    chosen = jnp.take_along_axis(transform_coefficients, picked, axis=1).astype(jnp.bfloat16)
    own_dense = densify(chosen, picked).astype(jnp.bfloat16)
    residual_momentum = (
        momentum.astype(jnp.float32) - decode_sparse(own_dense, cosines, cos_low)
    ).astype(jnp.bfloat16)
    slot_values = jnp.take(chosen, owner_span_order, axis=0)
    slot_spots = jnp.take(picked, owner_span_order, axis=0)
    shaped = (slot_values.reshape(owners, CH_OWN, TOPK), slot_spots.reshape(owners, CH_OWN, TOPK))
    partial_sum = owner_sum(
        (
            lax.all_to_all(shaped[0], "grp", split_axis=0, concat_axis=2, tiled=True),
            lax.all_to_all(shaped[1], "grp", split_axis=0, concat_axis=2, tiled=True),
        )
    )
    partial_sum = lax.psum(partial_sum, "rep")
    my_share = decode(partial_sum, cosines).astype(jnp.bfloat16)
    update = lax.all_gather(my_share, "grp", axis=0, tiled=True)
    return (update, residual_momentum)


LANES = 128
LOADS = 4
GATHER_BYTES = 2**20


def cosines_at(freq, place):
    turn = (freq * (2 * place + 1)) & (4 * BLOCK - 1)
    turn = jnp.where(turn > 2 * BLOCK, 4 * BLOCK - turn, turn)
    past = turn > BLOCK
    turn = jnp.where(past, 2 * BLOCK - turn, turn)
    angle = turn.astype(jnp.float32) * (math.pi / (2 * BLOCK))
    square = angle * angle
    value = jnp.full(square.shape, 1 / math.factorial(12), jnp.float32)
    for power in (10, 8, 6, 4, 2, 0):
        value = (-1) ** (power // 2) / math.factorial(power) + square * value
    scale = jnp.where(freq == 0, math.sqrt(1 / BLOCK), math.sqrt(2 / BLOCK))
    return (jnp.where(past, -value, value) * scale).astype(jnp.bfloat16)


def contract_lanes(left, right):
    return lax.dot_general(
        left, right, (((1,), (1,)), ((), ())), preferred_element_type=jnp.float32
    )


def matmul(left, right):
    return jnp.dot(left, right, preferred_element_type=jnp.float32)


def split(value):
    high = value.astype(jnp.bfloat16)
    return high, (value - high.astype(jnp.float32)).astype(jnp.bfloat16)


def exchange_kernel(
    groups,
    planes,
    order_hbm,
    momentum_hbm,
    picked_hbm,
    update_ref,
    residual_ref,
    order_ref,
    momentum_ref,
    picked_ref,
    rows_ref,
    wide_ref,
    twice_ref,
    pairs_ref,
    message,
    box,
    dense,
    summed,
    partial,
    row_side,
    column_side,
    weights,
    decoded,
    load_sem,
    send_sem,
    recv_sem,
    spot_sem,
    all_here,
):
    pltpu.make_async_copy(picked_hbm, picked_ref, load_sem).start()
    width = momentum_ref.shape[1] // LOADS
    for n in range(LOADS):
        piece = pl.ds(n * width, width)
        pltpu.make_async_copy(momentum_hbm.at[:, piece], momentum_ref.at[:, piece], send_sem).start()
    spans = momentum_ref.shape[0]
    entries = spans * TOPK
    chunks = BLOCK * BLOCK // LANES
    folds = chunks // 2
    in_tile = LANES // TOPK
    tiles = entries // LANES
    devices = groups * planes
    my_group, my_plane = lax.axis_index("grp"), lax.axis_index("rep")
    group_of = [lax.rem(my_group + step, groups) for step in range(groups)]
    early_planes, early_groups = max(1, planes // 2), max(1, groups // 2)
    early = early_planes * early_groups
    last = {"grp": jnp.int32(groups - 1), "rep": jnp.int32(planes - 1)}
    hubs = 2
    is_hub = jnp.logical_and(my_plane == 0, my_group < hubs)
    is_final = jnp.logical_and(my_plane == planes - 1, my_group >= groups - in_tile)
    is_last = jnp.logical_and(my_plane == planes - 1, my_group == groups - 1)
    is_early = jnp.logical_and(my_plane < early_planes, my_group < early_groups)

    def to_all(planes_of, groups_of, action):
        for z in planes_of:
            for g in groups_of:
                peer = {"grp": jnp.int32(g), "rep": jnp.int32(z)}
                is_me = jnp.logical_and(my_plane == z, my_group == g)
                pl.when(jnp.logical_not(is_me))(functools.partial(action, peer))

    def to_hubs(action):
        to_all(range(1), range(hubs), action)

    def to_others(action):
        to_all(range(1), range(hubs, early_groups), action)
        to_all(range(1, early_planes), range(early_groups), action)

    def to_early(action):
        to_hubs(action)
        to_others(action)

    def to_late(action):
        for z in range(early_planes, planes):
            for g in range(groups):
                peer = {"grp": group_of[g], "rep": jnp.int32(z)}
                if g:
                    action(peer)
                else:
                    pl.when(my_plane != z)(functools.partial(action, peer))
        to_all(range(early_planes), range(early_groups, groups), action)

    barrier = pltpu.get_barrier_semaphore()

    def signal(semaphore, peer):
        pl.semaphore_signal(semaphore, inc=1, device_id=peer, device_id_type=pl.DeviceIdType.MESH)

    @pl.when(is_early)
    def _():
        to_late(functools.partial(signal, barrier))
        to_early(functools.partial(signal, barrier))

    @pl.when(jnp.logical_not(jnp.logical_or(is_early, is_last)))
    def _():
        signal(barrier, last)

    def iotas(shape):
        return [lax.broadcasted_iota(jnp.int32, shape, d) for d in range(2)]

    line, freq = iotas((2 * folds, LANES))
    rows_ref[...] = cosines_at(freq % BLOCK, 2 * (line % folds) + line // folds).astype(jnp.float32)
    line, freq = iotas((BLOCK, BLOCK))
    pairs_ref[...] = cosines_at(freq, 2 * (line % chunks) + line // chunks)
    line, place = iotas((BLOCK, LANES))
    twice_ref[...] = cosines_at(line, place % BLOCK)
    wide_ref[...] = cosines_at(place % BLOCK, line).astype(jnp.float32)

    span, lane = iotas((spans, entries))
    turn = lax.rem(my_group, in_tile)
    block = (lane % LANES) // TOPK + in_tile - turn
    slot = lane // LANES * in_tile + jnp.where(block >= in_tile, block - in_tile, block)
    mine = span == slot

    @pl.when(is_last)
    def _():
        pl.semaphore_wait(barrier, devices - 1)
        to_late(functools.partial(signal, all_here))
        to_early(functools.partial(signal, all_here))

    pltpu.make_async_copy(picked_hbm, picked_ref, load_sem).wait()
    spread = jnp.concatenate([picked_ref[...]] * spans, axis=1)
    pltpu.make_async_copy(momentum_hbm, momentum_ref, send_sem).wait()
    spots = jnp.sum(jnp.where(mine, spread, 0), axis=0, keepdims=True)
    row_spot, col_spot = spots // BLOCK, spots % BLOCK

    def by_tile(row):
        return jnp.concatenate(
            [row[:, h * LANES : (h + 1) * LANES] for h in range(tiles)], axis=0
        ).astype(jnp.bfloat16)

    me = my_plane * groups + my_group
    batches = [(planes - 2) * groups, devices - in_tile, devices]
    batches = [b for b in sorted(set(batches)) if b]
    landing = sum(jnp.where(me >= b, 1, 0) for b in batches[:-1])
    value_part, spot_part = pl.ds(0, LANES), pl.ds(LANES, 2 * LANES)

    def copy_to(peer, lanes, semaphore):
        return pltpu.make_async_remote_copy(
            src_ref=message.at[:, lanes],
            dst_ref=box.at[me, :, lanes],
            send_sem=send_sem,
            recv_sem=semaphore,
            device_id=peer,
            device_id_type=pl.DeviceIdType.MESH,
        )

    def send(peer):
        copy_to(peer, pl.ds(0, 3 * LANES), recv_sem.at[landing]).start()

    def send_spots(peer):
        copy_to(peer, spot_part, spot_sem).start()

    def send_values(peer):
        copy_to(peer, value_part, recv_sem.at[landing]).start()

    message[:, LANES : 2 * LANES] = by_tile(row_spot.astype(jnp.float32))
    message[:, 2 * LANES :] = by_tile(col_spot.astype(jnp.float32))
    @pl.when(jnp.logical_and(is_final, jnp.logical_not(is_last)))
    def _():
        pl.semaphore_wait(barrier, early)

    pl.when(is_final)(lambda: to_hubs(send_spots))

    def looked_up(table, spot):
        height = table.shape[0]
        return jnp.concatenate(
            [
                jnp.take_along_axis(
                    table,
                    jnp.broadcast_to(spot[:, h * LANES : (h + 1) * LANES], (height, LANES)),
                    axis=1,
                    mode="promise_in_bounds",
                )
                for h in range(tiles)
            ],
            axis=1,
        )

    odd = jnp.where(row_spot % 2 == 1, -1.0, 1.0)
    wave = looked_up(wide_ref[...], col_spot)
    mirror = (wave * odd).astype(jnp.bfloat16)
    wave = wave.astype(jnp.bfloat16)
    waves = [jnp.concatenate([wave, mirror], axis=0), jnp.concatenate([mirror, wave], axis=0)]
    half_rows = folds * spans
    row_wave = looked_up(rows_ref[...], row_spot)
    row_waves = [row_wave[p * folds : (p + 1) * folds][:, None, :] for p in range(2)]


    def chunk(k):
        return momentum_ref[:, k * LANES : (k + 1) * LANES].astype(jnp.float32)

    left_lanes = lax.broadcasted_iota(jnp.int32, (spans, LANES), 1) < BLOCK

    def folded(p):
        pairs = [(chunk(k), chunk(chunks - 1 - k)) for k in range(folds)]
        return jnp.concatenate([jnp.where(left_lanes, pair[p], pair[1 - p]) for pair in pairs], axis=0)

    total = jnp.zeros((spans, entries), jnp.float32)
    for p in range(2):
        product = matmul(folded(p).astype(jnp.bfloat16), waves[p]).reshape(folds, spans, entries)
        total += jnp.sum(row_waves[p] * product, axis=0)
    chosen = jnp.sum(jnp.where(mine, total, 0.0), axis=0, keepdims=True)
    message[:, :LANES] = by_tile(chosen)

    @pl.when(jnp.logical_not(is_final))
    def _():
        pl.semaphore_wait(barrier, jnp.where(is_early, early - 1, early))
        to_hubs(send)

    pl.when(is_final)(lambda: to_hubs(send_values))
    to_others(send)

    pltpu.make_async_copy(message, box.at[me], recv_sem.at[landing]).start()

    pltpu.make_async_copy(order_hbm, order_ref, load_sem).start()
    chosen = chosen.astype(jnp.bfloat16).astype(jnp.float32)
    scaled = jnp.where(mine, chosen, 0.0)
    residuals = []
    for p in range(2):
        weight = row_waves[p] * scaled[None]
        residual = folded(p)
        for part in split(weight.reshape(half_rows, entries)):
            residual -= contract_lanes(part, waves[p])
        residuals.append(residual)
    for k in range(folds):
        pair = [residual[k * spans : (k + 1) * spans] for residual in residuals]
        for n, at in enumerate((k, chunks - 1 - k)):
            residual_ref[:, at * LANES : (at + 1) * LANES] = jnp.where(
                left_lanes, pair[n], pair[1 - n]
            ).astype(jnp.bfloat16)

    @pl.when(jnp.logical_not(is_last))
    def _():
        pl.semaphore_wait(all_here, 1)

    to_late(send)

    block = lax.broadcasted_iota(jnp.int32, (tiles, LANES), 1) // TOPK
    taken = [block == turn for turn in range(in_tile)]
    one, zero = jnp.ones((), jnp.bfloat16), jnp.zeros((), jnp.bfloat16)

    def await_part(n, lanes, semaphore):
        start = batches[n - 1] if n else 0
        landed = box.at[pl.ds(start, batches[n] - start), :, lanes]
        pltpu.make_async_copy(landed, landed, semaphore).wait()

    def parts_of(first, part):
        lanes = slice(part * LANES, (part + 1) * LANES)
        return [box[first + n, :, lanes].astype(jnp.float32) for n in range(in_tile)]

    def span_rows(parts, c):
        row = parts[0]
        for turn in range(1, in_tile):
            row = jnp.where(taken[(c + turn) % in_tile], parts[turn], row)
        return row

    def spread_out(row, freq, fill):
        return jnp.where(freq == row, fill, zero)

    def add_up(n, sums):
        await_part(n, pl.ds(0, 3 * LANES), recv_sem.at[n])
        firsts = list(range(batches[n - 1] if n else 0, batches[n], in_tile))
        for group in (firsts[m : m + 2] for m in range(0, len(firsts), 2)):
            pieces = [[parts_of(first, part) for part in range(3)] for first in group]
            freq = lax.broadcasted_iota(jnp.int32, (BLOCK, len(group) * LANES), 0)
            freq = freq.astype(jnp.float32).astype(jnp.bfloat16)
            for c in range(in_tile):
                value, row, column = (
                    jnp.concatenate([span_rows(piece[n], c) for piece in pieces], axis=1).astype(jnp.bfloat16)
                    for n in range(3)
                )
                for h in range(tiles):
                    left = spread_out(row[h : h + 1], freq, one)
                    right = spread_out(column[h : h + 1], freq, value[h : h + 1])
                    part = contract_lanes(left, right)
                    s = h * in_tile + c
                    sums[s] = part if sums[s] is None else sums[s] + part
        return sums

    lower = lax.broadcasted_iota(jnp.int32, (chunks, LANES), 1) < BLOCK

    def slot_matrices(sums):
        for s in range(spans):
            dense[s] = matmul(sums[s].astype(jnp.bfloat16), twice_ref[...]).astype(jnp.bfloat16)
        for s in range(spans):
            full = matmul(pairs_ref[...], dense[order_ref[s]])
            yield s, jnp.where(lower, full[:chunks], full[chunks:])

    sums = [None] * spans
    for n in range(len(batches) - 1):
        sums = add_up(n, sums)
    for s in range(spans):
        summed[s] = sums[s]
    pltpu.make_async_copy(order_hbm, order_ref, load_sem).wait()

    @pl.when(jnp.logical_not(is_hub))
    def _():
        for s, matrix in slot_matrices(add_up(len(batches) - 1, [summed[s] for s in range(spans)])):
            decoded[pl.ds(s, chunks, stride=spans), :] = matrix

    @pl.when(is_hub)
    def _():
        for s, matrix in slot_matrices([summed[s] for s in range(spans)]):
            partial[s] = matrix
        await_part(len(batches) - 1, spot_part, spot_sem)
        freq = lax.broadcasted_iota(jnp.int32, (BLOCK, entries), 0)
        freq = freq.astype(jnp.float32).astype(jnp.bfloat16)
        rows, columns = (parts_of(devices - in_tile, part) for part in (1, 2))
        for c in range(in_tile):
            row, column = (
                jnp.concatenate([span_rows(parts, c)[h : h + 1] for h in range(tiles)], axis=1).astype(jnp.bfloat16)
                for parts in (rows, columns)
            )
            left = matmul(pairs_ref[...], spread_out(row, freq, one)).astype(jnp.bfloat16)
            right = matmul(wide_ref[:, :BLOCK].astype(jnp.bfloat16), spread_out(column, freq, one)).astype(jnp.bfloat16)
            for h in range(tiles):
                row_side[h * in_tile + c] = left[:, h * LANES : (h + 1) * LANES]
                column_side[h * in_tile + c] = right[:, h * LANES : (h + 1) * LANES]
        await_part(len(batches) - 1, value_part, recv_sem.at[len(batches) - 1])
        values = parts_of(devices - in_tile, 0)
        for c in range(in_tile):
            value = span_rows(values, c)
            for h in range(tiles):
                weights[h * in_tile + c] = value[h : h + 1]
        for s in range(spans):
            span = order_ref[s]
            left = row_side[span] * jnp.broadcast_to(weights[span], (BLOCK, LANES)).astype(jnp.bfloat16)
            right = column_side[span]
            full = contract_lanes(left, jnp.concatenate([right, right], axis=0))
            decoded[pl.ds(s, chunks, stride=spans), :] = partial[s] + jnp.where(lower, full[:chunks], full[chunks:])

    for k in range(chunks):
        update_ref[:, k * LANES : (k + 1) * LANES] = decoded[
            k * spans : (k + 1) * spans, :
        ].astype(jnp.bfloat16)
    for _ in range(devices - 1):
        copy_to(last, pl.ds(0, 3 * LANES), recv_sem.at[landing]).wait_send()


def store_kernel(update_ref, residual_ref, update_hbm, residual_hbm, both, sem):
    pltpu.make_async_copy(residual_ref, residual_hbm, sem).start()
    pltpu.make_async_copy(update_ref, update_hbm, sem).start()
    pltpu.make_async_copy(both, both, sem).wait()


def local_small(groups, planes, momentum, picked, owner_span_order):
    spans = momentum.shape[0]
    chunks = BLOCK * BLOCK // LANES
    operands = [owner_span_order, momentum, picked]
    anywhere = pl.BlockSpec(memory_space=pl.ANY)
    vmem = pl.BlockSpec(memory_space=pltpu.VMEM)
    devices = groups * planes
    tile_shape = (spans * TOPK // LANES, 3 * LANES)
    results = pl.pallas_call(
        functools.partial(exchange_kernel, groups, planes),
        out_shape=[pltpu.VMEM(momentum.shape, jnp.bfloat16)] * 2,
        in_specs=[anywhere] * len(operands),
        out_specs=[vmem] * 2,
        scratch_shapes=[
            pltpu.SMEM(owner_span_order.shape, jnp.int32),
            pltpu.VMEM(momentum.shape, momentum.dtype),
            pltpu.VMEM(picked.shape, picked.dtype),
            pltpu.VMEM((chunks, LANES), jnp.float32),
            pltpu.VMEM((BLOCK, LANES), jnp.float32),
            pltpu.VMEM((BLOCK, LANES), jnp.bfloat16),
            pltpu.VMEM((BLOCK, BLOCK), jnp.bfloat16),
            pltpu.VMEM(tile_shape, jnp.bfloat16),
            pltpu.VMEM((devices, *tile_shape), jnp.bfloat16),
            pltpu.VMEM((spans, BLOCK, LANES), jnp.bfloat16),
            pltpu.VMEM((spans, BLOCK, BLOCK), jnp.float32),
            pltpu.VMEM((spans, chunks, LANES), jnp.float32),
            pltpu.VMEM((spans, BLOCK, LANES), jnp.bfloat16),
            pltpu.VMEM((spans, BLOCK, LANES), jnp.bfloat16),
            pltpu.VMEM((spans, 1, LANES), jnp.float32),
            pltpu.VMEM((chunks * spans, LANES), jnp.float32),
            pltpu.SemaphoreType.DMA,
            pltpu.SemaphoreType.DMA,
            pltpu.SemaphoreType.DMA((3,)),
            pltpu.SemaphoreType.DMA,
            pltpu.SemaphoreType.REGULAR,
        ],
        compiler_params=pltpu.CompilerParams(collective_id=0, has_side_effects=True),
    )(*operands)
    return pl.pallas_call(
        store_kernel,
        out_shape=[jax.ShapeDtypeStruct(momentum.shape, jnp.bfloat16)] * 2,
        in_specs=[vmem] * 2,
        out_specs=[anywhere] * 2,
        scratch_shapes=[pltpu.VMEM((2, *momentum.shape), jnp.bfloat16), pltpu.SemaphoreType.DMA],
    )(*[pltpu.with_memory_space_constraint(result, pltpu.VMEM) for result in results])


def local(groups, planes, momentum, picked, owner_span_order):
    entries = momentum.shape[0] * TOPK
    if entries % LANES == 0 and planes > 1 and groups > LANES // TOPK and groups % (LANES // TOPK) == 0 and groups * planes * entries * 8 <= GATHER_BYTES:
        return local_small(groups, planes, momentum, picked, owner_span_order)
    return local_large(momentum, picked, owner_span_order)


def solution(mesh):
    return jax.shard_map(
        functools.partial(local, mesh.shape["grp"], mesh.shape["rep"]),
        mesh=mesh,
        in_specs=(P(("grp", "rep"), None), P(("grp", "rep"), None), P()),
        out_specs=(P(), P(("grp", "rep"), None)),
        check_vma=False,
    )
```
